16 devices in a mesh: dp: 2 (over y, z), ep: 8 (over x, core).
Axes of the slice: x: 4, y: 2, z: 1, core: 2. Of those that a mesh axis runs over, the one named last changes fastest.
The devices are a block of a 4x4x8 slice.
Arguments:
- tokens: bfloat16 [2, 32, 512, 1536], P(None, ('dp', 'ep')), parts along dimension 1
- expert_ids: int32 [2, 16384, 6], P(None, ('dp', 'ep')), parts along dimension 1
- route_weights: float32 [2, 16384, 6], P(None, ('dp', 'ep')), parts along dimension 1
- attn_norm: bfloat16 [1536], replicated
- w_query: bfloat16 [1536, 12, 128], replicated
- w_key: bfloat16 [1536, 12, 128], replicated
- w_value: bfloat16 [1536, 12, 128], replicated
- w_out: bfloat16 [12, 128, 1536], replicated
- ffn_norm: bfloat16 [1536], replicated
- w_gate: bfloat16 [64, 1536, 512], P('ep')
- w_up: bfloat16 [64, 1536, 512], P('ep')
- w_down: bfloat16 [64, 512, 1536], P('ep')
- shared_gate: bfloat16 [1536, 1024], replicated
- shared_up: bfloat16 [1536, 1024], replicated
- shared_down: bfloat16 [1024, 1536], replicated
Outputs:
- output: bfloat16 [2, 32, 512, 1536], P(None, ('dp', 'ep')), parts along dimension 1
There are 2 independent parts. The reference program is written for one: setup_inputs(seed, part) draws one part's arguments, and reference() takes and returns one part's arrays. A program takes and returns all parts, laid end to end along the dimension named above; an argument that names none is the same for every part.
All inputs are finite; a program needn't handle non-finite values.
Results may differ from the reference program's by a relative error of at most 0.00977925.
Values are sent between devices in bfloat16 or wider.
A program may use at most 768 MiB of HBM per device.

```python
import jax
import jax.numpy as jnp
import numpy as np
from jax import lax

TOKENS = 1024
SEQ = 512
D_MODEL = 1536
HEADS = 12
HEAD_DIM = 128
EXPERTS = 64
TOP = 6
FF = 512
SHARED_FF = 1024
GROUP = 8
CAPACITY = 192
NORM_EPS = 1e-6


def load_profile():
    total_rows = TOKENS * TOP
    rest_rows = total_rows - CAPACITY
    weight_list = [3 * (EXPERTS - 1) - 2 * rank_pos for rank_pos in range(EXPERTS - 1)]
    weight_sum = sum(weight_list)
    count_list = [rest_rows * weight_val // weight_sum for weight_val in weight_list]
    extra_units = rest_rows - sum(count_list)
    count_list = [count_val + (1 if rank_pos < extra_units else 0) for rank_pos, count_val in enumerate(count_list)]
    return [CAPACITY] + count_list


def draw_routing(base_key):
    rank_ids = np.repeat(np.arange(EXPERTS), np.array(load_profile()))

    def one_micro(micro_key):
        sub_keys = jax.random.split(micro_key)
        expert_of_rank = jax.random.permutation(sub_keys[0], EXPERTS)
        id_grid = expert_of_rank[rank_ids].reshape(TOP, TOKENS).T
        device_keys = jax.random.split(sub_keys[1], GROUP)

        def one_device(device_key):
            return id_grid[jax.random.permutation(device_key, TOKENS)]

        return jax.vmap(one_device)(device_keys).reshape(GROUP * TOKENS, TOP)

    return jax.vmap(one_micro)(jax.random.split(base_key, 2)).astype(jnp.int32)


def draw_normal(sub_key, array_shape, std_scale):
    return (jax.random.normal(sub_key, array_shape, jnp.float32) * std_scale).astype(jnp.bfloat16)


def setup_inputs(seed: int = 0, part: int = 0) -> dict:
    weight_keys = jax.random.split(jax.random.key(seed), 12)
    part_keys = jax.random.split(jax.random.fold_in(jax.random.key(seed + 1), part), 3)
    n_rows = GROUP * TOKENS
    attn_width = HEADS * HEAD_DIM
    return {
        "tokens": draw_normal(part_keys[0], (2, n_rows // SEQ, SEQ, D_MODEL), 1.0),
        "expert_ids": draw_routing(part_keys[1]),
        "route_weights": jax.nn.softmax(jax.random.normal(part_keys[2], (2, n_rows, TOP), jnp.float32), axis=-1),
        "attn_norm": jax.random.uniform(weight_keys[0], (D_MODEL,), jnp.float32, 0.5, 1.5).astype(jnp.bfloat16),
        "w_query": draw_normal(weight_keys[1], (D_MODEL, HEADS, HEAD_DIM), D_MODEL ** -0.5),
        "w_key": draw_normal(weight_keys[2], (D_MODEL, HEADS, HEAD_DIM), D_MODEL ** -0.5),
        "w_value": draw_normal(weight_keys[3], (D_MODEL, HEADS, HEAD_DIM), D_MODEL ** -0.5),
        "w_out": draw_normal(weight_keys[4], (HEADS, HEAD_DIM, D_MODEL), attn_width ** -0.5),
        "ffn_norm": jax.random.uniform(weight_keys[5], (D_MODEL,), jnp.float32, 0.5, 1.5).astype(jnp.bfloat16),
        "w_gate": draw_normal(weight_keys[6], (EXPERTS, D_MODEL, FF), D_MODEL ** -0.5),
        "w_up": draw_normal(weight_keys[7], (EXPERTS, D_MODEL, FF), D_MODEL ** -0.5),
        "w_down": draw_normal(weight_keys[8], (EXPERTS, FF, D_MODEL), 2.0 * FF ** -0.5),
        "shared_gate": draw_normal(weight_keys[9], (D_MODEL, SHARED_FF), D_MODEL ** -0.5),
        "shared_up": draw_normal(weight_keys[10], (D_MODEL, SHARED_FF), D_MODEL ** -0.5),
        "shared_down": draw_normal(weight_keys[11], (SHARED_FF, D_MODEL), SHARED_FF ** -0.5),
    }


def rms_norm(in_vals, norm_gain):
    wide_vals = in_vals.astype(jnp.float32)
    inv_rms = lax.rsqrt(jnp.mean(wide_vals * wide_vals, axis=-1, keepdims=True) + NORM_EPS)
    return (wide_vals * inv_rms * norm_gain.astype(jnp.float32)).astype(jnp.bfloat16)


def attention_block(seq_rows, attn_norm, w_query, w_key, w_value, w_out):
    n_seq = seq_rows.shape[0]
    normed = rms_norm(seq_rows, attn_norm).reshape(n_seq * SEQ, D_MODEL)

    def project(weight):
        proj_rows = jnp.dot(normed, weight.reshape(D_MODEL, HEADS * HEAD_DIM), preferred_element_type=jnp.float32)
        return proj_rows.astype(jnp.bfloat16).reshape(n_seq, SEQ, HEADS, HEAD_DIM)

    queries = project(w_query)
    key_rows = project(w_key)
    value_rows = project(w_value)
    scores = jnp.einsum("bqhe,bkhe->bhqk", queries.astype(jnp.float32), key_rows.astype(jnp.float32)) * HEAD_DIM ** -0.5
    causal = jnp.arange(SEQ)[:, None] >= jnp.arange(SEQ)[None, :]
    attn_probs = jax.nn.softmax(jnp.where(causal, scores, -jnp.inf), axis=-1).astype(jnp.bfloat16)
    head_mix = jnp.einsum("bhqk,bkhe->bqhe", attn_probs.astype(jnp.float32), value_rows.astype(jnp.float32)).astype(jnp.bfloat16)
    attn_out = jnp.dot(head_mix.reshape(n_seq * SEQ, HEADS * HEAD_DIM), w_out.reshape(HEADS * HEAD_DIM, D_MODEL), preferred_element_type=jnp.float32)
    return (seq_rows.astype(jnp.float32) + attn_out.reshape(n_seq, SEQ, D_MODEL)).astype(jnp.bfloat16)


def swiglu(in_rows, gate_w, up_w, down_w):
    gate_act = jnp.dot(in_rows, gate_w, preferred_element_type=jnp.float32)
    up_act = jnp.dot(in_rows, up_w, preferred_element_type=jnp.float32)
    hidden = (jax.nn.silu(gate_act) * up_act).astype(jnp.bfloat16)
    return jnp.dot(hidden, down_w, preferred_element_type=jnp.float32).astype(jnp.bfloat16)


def route_plan(flat_ids, slot_cap):
    n_rows = flat_ids.shape[0]
    sort_order = jnp.argsort(flat_ids, stable=True).astype(jnp.int32)
    counts = jnp.bincount(flat_ids, length=EXPERTS)
    starts = jnp.cumsum(counts) - counts
    sorted_rank = jnp.zeros((n_rows,), jnp.int32).at[sort_order].set(jnp.arange(n_rows, dtype=jnp.int32))
    slot_ids = sorted_rank - starts[flat_ids]
    src_pos = sort_order[jnp.minimum(starts[:, None] + jnp.arange(slot_cap)[None, :], n_rows - 1)]
    return slot_ids, src_pos


def reference(tokens, expert_ids, route_weights, attn_norm, w_query, w_key, w_value, w_out, ffn_norm, w_gate, w_up, w_down, shared_gate, shared_up, shared_down):
    def one_micro(micro_inputs):
        micro_tok, micro_ids, micro_weights = micro_inputs
        dev_seqs = micro_tok.reshape(GROUP, TOKENS // SEQ, SEQ, D_MODEL)
        residual = lax.map(lambda dev_rows: attention_block(dev_rows, attn_norm, w_query, w_key, w_value, w_out), dev_seqs)
        residual = residual.reshape(GROUP * TOKENS, D_MODEL)
        normed = rms_norm(residual, ffn_norm)
        shared_out = swiglu(normed, shared_gate, shared_up, shared_down)
        flat_ids = micro_ids.reshape(-1)
        slot_cap = GROUP * CAPACITY
        slot_ids, src_pos = route_plan(flat_ids, slot_cap)
        expert_in = normed[src_pos // TOP]
        expert_out = lax.map(lambda packed: swiglu(packed[0], packed[1], packed[2], packed[3]), (expert_in, w_gate, w_up, w_down))
        picked = expert_out.reshape(EXPERTS * slot_cap, D_MODEL)[flat_ids * slot_cap + slot_ids]
        picked = picked.reshape(GROUP * TOKENS, TOP, D_MODEL)
        routed = jnp.sum(picked.astype(jnp.float32) * micro_weights[:, :, None], axis=1)
        layer_rows = residual.astype(jnp.float32) + shared_out.astype(jnp.float32) + routed
        return layer_rows.astype(jnp.bfloat16).reshape(micro_tok.shape)

    return lax.map(one_micro, (tokens, expert_ids, route_weights))
```

```python
import functools

import jax
import jax.numpy as jnp
from jax import lax
from jax.experimental import pallas as pl
from jax.experimental.pallas import tpu as pltpu
from jax.sharding import PartitionSpec as P

NORM_EPS = 1e-6
CAP_FACTOR = 2
SLOT_ALIGN = 8
SEG = 16
ROWS = 256
VMEM_LIMIT = 64_000_000


def capacity_of(n_tok, top_count, experts):
    return SLOT_ALIGN * ((CAP_FACTOR * n_tok * top_count + SLOT_ALIGN * experts - 1) // (SLOT_ALIGN * experts))


def rms_norm(in_vals, norm_gain):
    wide_vals = in_vals.astype(jnp.float32)
    inv_rms = lax.rsqrt(jnp.mean(wide_vals * wide_vals, axis=-1, keepdims=True) + NORM_EPS)
    return (wide_vals * inv_rms * norm_gain.astype(jnp.float32)).astype(jnp.bfloat16)


def attention_block(seq_rows, attn_norm, w_query, w_key, w_value, w_out):
    normed = rms_norm(seq_rows, attn_norm)
    queries = jnp.einsum("...sd,dhe->...she", normed, w_query, preferred_element_type=jnp.float32).astype(jnp.bfloat16)
    key_rows = jnp.einsum("...sd,dhe->...she", normed, w_key, preferred_element_type=jnp.float32).astype(jnp.bfloat16)
    value_rows = jnp.einsum("...sd,dhe->...she", normed, w_value, preferred_element_type=jnp.float32).astype(jnp.bfloat16)
    seq_len = seq_rows.shape[-2]
    scores = jnp.einsum("...qhe,...khe->...hqk", queries, key_rows, preferred_element_type=jnp.float32) * (w_query.shape[-1] ** -0.5)
    causal = jnp.arange(seq_len)[:, None] >= jnp.arange(seq_len)[None, :]
    attn_probs = jax.nn.softmax(jnp.where(causal, scores, -jnp.inf), axis=-1).astype(jnp.bfloat16)
    head_mix = jnp.einsum("...hqk,...khe->...qhe", attn_probs, value_rows, preferred_element_type=jnp.float32).astype(jnp.bfloat16)
    attn_out = jnp.einsum("...qhe,hed->...qd", head_mix, w_out, preferred_element_type=jnp.float32)
    return (seq_rows.astype(jnp.float32) + attn_out).astype(jnp.bfloat16)


def swiglu(in_rows, gate_w, up_w, down_w):
    gate_act = jnp.dot(in_rows, gate_w, preferred_element_type=jnp.float32)
    up_act = jnp.dot(in_rows, up_w, preferred_element_type=jnp.float32)
    hidden = (jax.nn.silu(gate_act) * up_act).astype(jnp.bfloat16)
    return jnp.dot(hidden, down_w, preferred_element_type=jnp.float32).astype(jnp.bfloat16)


def route_tables(local_ids, weights, n_local):
    n_src, _, n_tok = local_ids.shape
    hits = local_ids[:, :, None, :] == jnp.arange(n_local)[None, None, :, None]
    mask = jnp.any(hits, axis=1)
    upper = (jnp.arange(n_tok)[:, None] <= jnp.arange(n_tok)[None, :]).astype(jnp.bfloat16)
    running = jnp.dot(mask.astype(jnp.bfloat16).reshape(n_src * n_local, n_tok), upper, preferred_element_type=jnp.float32)
    running = running.astype(jnp.int32).reshape(n_src, n_local, n_tok)
    counts = running[:, :, -1]
    padded = (counts + SEG - 1) // SEG * SEG
    before_e = (jnp.arange(n_local)[:, None] < jnp.arange(n_local)[None, :]).astype(jnp.int32)
    before_s = (jnp.arange(n_src)[:, None] < jnp.arange(n_src)[None, :]).astype(jnp.int32)
    offs = jnp.sum(padded[:, :, None] * before_e[None], axis=1)
    places = jnp.sum(padded[:, None, :] * before_s[:, :, None], axis=0)
    slot_of = offs[:, :, None] + running - 1
    slots = jnp.sum(jnp.where(hits, slot_of[:, None] + 1, 0), axis=2) - 1
    table = jnp.concatenate([offs.reshape(-1), padded.reshape(-1), places.reshape(-1), jnp.sum(padded, axis=0), jnp.sum(padded, axis=1)])
    pad_rows = jnp.full((n_src, 8 - slots.shape[1], n_tok), -1, jnp.int32)
    slot_rows = jnp.concatenate([slots, pad_rows], axis=1)
    cols = jnp.concatenate([slots.astype(jnp.float32), weights], axis=1).transpose(0, 2, 1)
    return table, slot_rows, cols


def gather_kernel(n_src, n_local, top_count, table_ref, slots_ref, z_ref, x_ref):
    src = pl.program_id(0)
    n_tok = z_ref.shape[0]
    total = table_ref[3 * n_src * n_local + n_local + src]

    def chunk(c, carry):
        base = c * ROWS
        rows = lax.broadcasted_iota(jnp.int32, (ROWS, n_tok), 0) + base
        hit = rows == slots_ref[0, 0:1, :]
        for j in range(1, top_count):
            hit = hit | (rows == slots_ref[0, j : j + 1, :])
        pick = jnp.where(hit, 1.0, 0.0).astype(jnp.bfloat16)
        got = jnp.dot(pick, z_ref[...], preferred_element_type=jnp.float32)
        x_ref[0, pl.ds(pl.multiple_of(base, ROWS), ROWS), :] = got.astype(jnp.bfloat16)
        return carry

    lax.fori_loop(0, (total + ROWS - 1) // ROWS, chunk, 0)


def gather_rows(table, slot_rows, z_all, n_local, top_count, max_rows):
    n_src = slot_rows.shape[0]
    n_tok = z_all.shape[0] // n_src
    d_model = z_all.shape[1]
    return pl.pallas_call(
        functools.partial(gather_kernel, n_src, n_local, top_count),
        out_shape=jax.ShapeDtypeStruct((n_src, max_rows, d_model), jnp.bfloat16),
        grid_spec=pltpu.PrefetchScalarGridSpec(
            num_scalar_prefetch=1,
            grid=(n_src,),
            in_specs=[
                pl.BlockSpec((1, 8, n_tok), lambda s, t: (s, 0, 0)),
                pl.BlockSpec((n_tok, d_model), lambda s, t: (s, 0)),
            ],
            out_specs=pl.BlockSpec((1, max_rows, d_model), lambda s, t: (s, 0, 0)),
        ),
        compiler_params=pltpu.CompilerParams(dimension_semantics=("arbitrary",), vmem_limit_bytes=VMEM_LIMIT),
        cost_estimate=pl.CostEstimate(flops=2 * 6656 * n_tok * d_model, bytes_accessed=60_000_000, transcendentals=0),
        name="gather_rows",
    )(table, slot_rows, z_all)


def expert_kernel(n_src, n_local, table_ref, x_hbm, ga, ua, da, gb, ub, db, y_hbm, x_buf, y_buf, in_sems, out_sems):
    step = pl.program_id(0)
    n_seg = n_src * n_local
    bits = in_sems.shape[2]

    def pieces(which, act):
        slot = lax.rem(which, 2)
        for s in range(n_src):
            off = table_ref[s * n_local + which]
            size = table_ref[n_seg + s * n_local + which]
            place = table_ref[2 * n_seg + s * n_local + which]
            units = size // SEG
            done = 0
            for b in reversed(range(bits)):
                length = SEG << b
                at_hbm = pl.multiple_of(off + done, SEG)
                at_buf = pl.multiple_of(place + done, SEG)
                has = (units >> b) & 1

                @pl.when(has == 1)
                def _():
                    act(slot, s, b, at_hbm, at_buf, length)

                done = done + has * length

    def in_copy(slot, s, b, at_hbm, at_buf, length):
        return pltpu.make_async_copy(x_hbm.at[s, pl.ds(at_hbm, length)], x_buf.at[slot, pl.ds(at_buf, length)], in_sems.at[slot, s, b])

    def out_copy(slot, s, b, at_hbm, at_buf, length):
        return pltpu.make_async_copy(y_buf.at[slot, pl.ds(at_buf, length)], y_hbm.at[s, pl.ds(at_hbm, length)], out_sems.at[slot, s, b])

    @pl.when(step == 0)
    def _():
        pieces(step, lambda *a: in_copy(*a).start())

    @pl.when(step + 1 < n_local)
    def _():
        pieces(step + 1, lambda *a: in_copy(*a).start())

    pieces(step, lambda *a: in_copy(*a).wait())

    @pl.when(step >= 2)
    def _():
        pieces(step - 2, lambda *a: out_copy(*a).wait())

    slot = lax.rem(step, 2)
    total = table_ref[3 * n_seg + step]
    n_blocks = (total + ROWS - 1) // ROWS

    def run(gate, up, down):
        def block(c, carry):
            rows = pl.ds(pl.multiple_of(c * ROWS, ROWS), ROWS)
            x = x_buf[slot, rows, :]
            g = jnp.dot(x, gate[0], preferred_element_type=jnp.float32)
            u = jnp.dot(x, up[0], preferred_element_type=jnp.float32)
            h = (g * jax.nn.sigmoid(g) * u).astype(jnp.bfloat16)
            y_buf[slot, rows, :] = jnp.dot(h, down[0], preferred_element_type=jnp.float32).astype(jnp.bfloat16)
            return carry

        lax.fori_loop(0, n_blocks, block, 0)

    @pl.when(step < n_local // 2)
    def _():
        run(ga, ua, da)

    @pl.when(step >= n_local // 2)
    def _():
        run(gb, ub, db)

    pieces(step, lambda *a: out_copy(*a).start())

    @pl.when(step == n_local - 1)
    def _():
        pieces(step - 1, lambda *a: out_copy(*a).wait())
        pieces(step, lambda *a: out_copy(*a).wait())


def expert_rows(table, x_rows, own, other, slot_cap):
    n_src, max_rows, d_model = x_rows.shape
    half, _, width = own[0].shape
    n_local = 2 * half
    buf_rows = -(-n_src * slot_cap // ROWS) * ROWS
    bits = (slot_cap // SEG).bit_length()
    own_at = lambda l, t: (jnp.minimum(l, half - 1), 0, 0)
    other_at = lambda l, t: (jnp.maximum(l - half, 0), 0, 0)
    return pl.pallas_call(
        functools.partial(expert_kernel, n_src, n_local),
        out_shape=jax.ShapeDtypeStruct(x_rows.shape, jnp.bfloat16),
        grid_spec=pltpu.PrefetchScalarGridSpec(
            num_scalar_prefetch=1,
            grid=(n_local,),
            in_specs=[
                pl.BlockSpec(memory_space=pl.ANY),
                pl.BlockSpec((1, d_model, width), own_at),
                pl.BlockSpec((1, d_model, width), own_at),
                pl.BlockSpec((1, width, d_model), own_at),
                pl.BlockSpec((1, d_model, width), other_at),
                pl.BlockSpec((1, d_model, width), other_at),
                pl.BlockSpec((1, width, d_model), other_at),
            ],
            out_specs=pl.BlockSpec(memory_space=pl.ANY),
            scratch_shapes=[
                pltpu.VMEM((2, buf_rows, d_model), jnp.bfloat16),
                pltpu.VMEM((2, buf_rows, d_model), jnp.bfloat16),
                pltpu.SemaphoreType.DMA((2, n_src, bits)),
                pltpu.SemaphoreType.DMA((2, n_src, bits)),
            ],
        ),
        compiler_params=pltpu.CompilerParams(dimension_semantics=("arbitrary",), vmem_limit_bytes=VMEM_LIMIT),
        cost_estimate=pl.CostEstimate(flops=2 * 8192 * d_model * width * 3, bytes_accessed=115_000_000, transcendentals=0),
        name="expert_rows",
    )(table, x_rows, *own, *other)


def combine_kernel(n_src, n_local, top_count, table_ref, cols_ref, y_ref, out_ref, slot_bc, weight_bc):
    src = pl.program_id(0)
    n_tok = out_ref.shape[0]
    total = table_ref[3 * n_src * n_local + n_local + src]
    lanes = 128
    for j in range(top_count):
        slot_bc[j] = jnp.broadcast_to(cols_ref[0, :, j : j + 1], (n_tok, lanes))
        weight_bc[j] = jnp.broadcast_to(cols_ref[0, :, top_count + j : top_count + j + 1], (n_tok, lanes))
    out_ref[...] = jnp.zeros_like(out_ref)

    def chunk(c, carry):
        base = c * ROWS
        rows = pl.ds(pl.multiple_of(base, ROWS), ROWS)
        y = y_ref[0, rows, :]
        y_at = lax.broadcasted_iota(jnp.int32, y.shape, 0) + base
        y = jnp.where(y_at < total, y, jnp.zeros_like(y))

        def tokens(i, inner):
            tok = pl.ds(pl.multiple_of(i * ROWS, ROWS), ROWS)
            parts = [[], [], []]
            for half in range(ROWS // lanes):
                lane_at = (lax.broadcasted_iota(jnp.int32, (ROWS, lanes), 1) + (base + half * lanes)).astype(jnp.float32)
                coef = jnp.zeros((ROWS, lanes), jnp.float32)
                for j in range(top_count):
                    coef = jnp.where(slot_bc[j, tok, :] == lane_at, weight_bc[j, tok, :], coef)
                high = coef.astype(jnp.bfloat16)
                rest = coef - high.astype(jnp.float32)
                mid = rest.astype(jnp.bfloat16)
                low = (rest - mid.astype(jnp.float32)).astype(jnp.bfloat16)
                for part, val in zip(parts, (high, mid, low)):
                    part.append(val)
            high, mid, low = (jnp.concatenate(part, axis=1) for part in parts)
            acc = jnp.dot(low, y, preferred_element_type=jnp.float32)
            acc = acc + jnp.dot(mid, y, preferred_element_type=jnp.float32)
            acc = acc + jnp.dot(high, y, preferred_element_type=jnp.float32)
            out_ref[tok, :] += acc
            return inner

        lax.fori_loop(0, n_tok // ROWS, tokens, 0)
        return carry

    lax.fori_loop(0, (total + ROWS - 1) // ROWS, chunk, 0)


def combine_rows(table, cols, y_rows, n_local, top_count):
    n_src, max_rows, d_model = y_rows.shape
    n_tok = cols.shape[1]
    return pl.pallas_call(
        functools.partial(combine_kernel, n_src, n_local, top_count),
        out_shape=jax.ShapeDtypeStruct((n_src * n_tok, d_model), jnp.float32),
        grid_spec=pltpu.PrefetchScalarGridSpec(
            num_scalar_prefetch=1,
            grid=(n_src,),
            in_specs=[
                pl.BlockSpec((1, n_tok, 2 * top_count), lambda s, t: (s, 0, 0)),
                pl.BlockSpec((1, max_rows, d_model), lambda s, t: (s, 0, 0)),
            ],
            out_specs=pl.BlockSpec((n_tok, d_model), lambda s, t: (s, 0)),
            scratch_shapes=[
                pltpu.VMEM((top_count, n_tok, 128), jnp.float32),
                pltpu.VMEM((top_count, n_tok, 128), jnp.float32),
            ],
        ),
        compiler_params=pltpu.CompilerParams(dimension_semantics=("arbitrary",), vmem_limit_bytes=VMEM_LIMIT),
        cost_estimate=pl.CostEstimate(flops=6 * 7168 * n_tok * d_model, bytes_accessed=62_000_000, transcendentals=0),
        name="combine_rows",
    )(table, cols, y_rows)


def solution(mesh):
    group_size = mesh.shape["ep"]
    n_src = group_size // 2
    ring_groups = [[2 * k + core for k in range(n_src)] for core in range(2)]
    pair_perm = [(k, k ^ 1) for k in range(group_size)]

    def device_step(tokens, expert_ids, route_weights, attn_norm, w_query, w_key, w_value, w_out, ffn_norm, w_gate, w_up, w_down, shared_gate, shared_up, shared_down):
        n_micro, n_seq, seq_len, d_model = tokens.shape
        n_tok = n_seq * seq_len
        top_count = expert_ids.shape[-1]
        half = w_gate.shape[0]
        n_local = 2 * half
        slot_cap = capacity_of(n_tok, top_count, half * group_size)
        max_rows = n_local * slot_cap
        me = lax.axis_index("ep")

        own = (w_gate, w_up, w_down)
        other = tuple(lax.ppermute(w, "ep", pair_perm) for w in own)

        meta = jnp.concatenate([expert_ids.astype(jnp.float32).transpose(0, 2, 1), route_weights.transpose(0, 2, 1), jnp.zeros((n_micro, 16 - 2 * top_count, n_tok), jnp.float32)], axis=1)
        meta = lax.all_gather(meta.reshape(n_micro * 16, n_tok), "ep", axis=0, tiled=True)
        meta = meta.reshape(n_src, 2, n_micro, 16, n_tok)
        meta = lax.dynamic_index_in_dim(meta, me % 2, axis=1, keepdims=False)
        ids = meta[:, :, :top_count].astype(jnp.int32)
        all_weights = meta[:, :, top_count : 2 * top_count]
        from_own = ids - half * me
        from_other = ids - half * (me ^ 1)
        local_ids = jnp.where((from_own >= 0) & (from_own < half), from_own, jnp.where((from_other >= 0) & (from_other < half), from_other + half, -1))
        plans = [route_tables(local_ids[:, m], all_weights[:, m], n_local) for m in range(n_micro)]

        residuals, normeds, gathered = [], [], []
        for m in range(n_micro):
            residual = attention_block(tokens[m], attn_norm, w_query, w_key, w_value, w_out).reshape(n_tok, d_model)
            normed = rms_norm(residual, ffn_norm)
            residuals.append(residual)
            normeds.append(normed)
            gathered.append(lax.all_gather(normed, "ep", axis=0, tiled=True, axis_index_groups=ring_groups))
        outs = []
        for m in range(n_micro):
            table, slot_rows, cols = plans[m]
            x_rows = gather_rows(table, slot_rows, gathered[m], n_local, top_count, max_rows)
            y_rows = expert_rows(table, x_rows, own, other, slot_cap)
            partial = combine_rows(table, cols, y_rows, n_local, top_count)
            routed = lax.psum_scatter(partial, "ep", scatter_dimension=0, tiled=True, axis_index_groups=ring_groups)
            shared_out = swiglu(normeds[m], shared_gate, shared_up, shared_down)
            layer_rows = residuals[m].astype(jnp.float32) + shared_out.astype(jnp.float32) + routed
            outs.append(layer_rows.astype(jnp.bfloat16).reshape(n_seq, seq_len, d_model))
        return jnp.stack(outs)

    token_spec = P(None, ("dp", "ep"), None, None)
    route_spec = P(None, ("dp", "ep"), None)
    rep_spec = P()
    expert_spec = P("ep", None, None)
    in_specs = (token_spec, route_spec, route_spec, rep_spec, rep_spec, rep_spec, rep_spec, rep_spec, rep_spec, expert_spec, expert_spec, expert_spec, rep_spec, rep_spec, rep_spec)
    return jax.shard_map(device_step, mesh=mesh, in_specs=in_specs, out_specs=token_spec, check_vma=False)
```

```python
import functools

import jax
import jax.numpy as jnp
from jax import lax
from jax.experimental import pallas as pl
from jax.experimental.pallas import tpu as pltpu
from jax.sharding import PartitionSpec as P


NORM_EPS = 1e-6
CAP_FACTOR = 2
SLOT_ALIGN = 8
SEG = 16
ROWS = 256
VMEM_LIMIT = 64_000_000


def capacity_of(n_tok, top_count, experts):
    return SLOT_ALIGN * ((CAP_FACTOR * n_tok * top_count + SLOT_ALIGN * experts - 1) // (SLOT_ALIGN * experts))


def rms_norm(in_vals, norm_gain):
    wide_vals = in_vals.astype(jnp.float32)
    inv_rms = lax.rsqrt(jnp.mean(wide_vals * wide_vals, axis=-1, keepdims=True) + NORM_EPS)
    return (wide_vals * inv_rms * norm_gain.astype(jnp.float32)).astype(jnp.bfloat16)


def attention_kernel(gain_ref, ffn_gain_ref, x_ref, wq_ref, wk_ref, wv_ref, wo_ref, h_ref, z_ref, normed, acc):
    group, seq = pl.program_id(0), pl.program_id(1)
    seq_len, d_model = normed.shape[1:]
    per, _, head_dim = wq_ref.shape
    block = seq_len // 2

    @pl.when(group == 0)
    def _():
        normed[seq] = rms_norm(x_ref[0, seq], gain_ref[...])

    rows = normed[seq]
    project = lambda w_ref: jnp.dot(rows, jnp.concatenate([w_ref[i] for i in range(per)], axis=1), preferred_element_type=jnp.float32).astype(jnp.bfloat16)
    queries, key_rows, value_rows = project(wq_ref), project(wk_ref), project(wv_ref)
    above = lax.broadcasted_iota(jnp.int32, (block, block), 0) < lax.broadcasted_iota(jnp.int32, (block, block), 1)
    tops, ends = [], []
    for i in range(per):
        lanes = slice(i * head_dim, (i + 1) * head_dim)
        k, v = key_rows[:, lanes], value_rows[:, lanes]
        for part, outs in ((0, tops), (1, ends)):
            q = queries[part * block : (part + 1) * block, lanes]
            scores = lax.dot_general(q, k[: (part + 1) * block], (((1,), (1,)), ((), ())), preferred_element_type=jnp.float32) * (head_dim**-0.5)
            diag = jnp.where(above, -jnp.inf, scores[:, part * block :])
            scores = diag if part == 0 else jnp.concatenate([scores[:, :block], diag], axis=1)
            shifted = jnp.exp(scores - jnp.max(scores, axis=1, keepdims=True))
            probs = (shifted * (1.0 / jnp.sum(shifted, axis=1, keepdims=True))).astype(jnp.bfloat16)
            outs.append(jnp.dot(probs, v[: (part + 1) * block], preferred_element_type=jnp.float32).astype(jnp.bfloat16))
    mix = jnp.concatenate([jnp.concatenate(tops, axis=1), jnp.concatenate(ends, axis=1)], axis=0)
    added = jnp.dot(mix, wo_ref[...].reshape(per * head_dim, d_model), preferred_element_type=jnp.float32)

    @pl.when(group == 0)
    def _():
        acc[seq] = added

    @pl.when(group > 0)
    def _():
        acc[seq] += added

    @pl.when(group == pl.num_programs(0) - 1)
    def _():
        residual = (x_ref[0, seq].astype(jnp.float32) + acc[seq]).astype(jnp.bfloat16)
        h_ref[seq] = residual
        z_ref[seq] = rms_norm(residual, ffn_gain_ref[...])


def attention_rows(tokens, micro, first, n_seq, gains, weights):
    _, _, seq_len, d_model = tokens.shape
    n_heads, _, head_dim = weights[0].shape
    per = 2
    out = jax.ShapeDtypeStruct((n_seq, seq_len, d_model), jnp.bfloat16)
    whole = pl.BlockSpec((n_seq, seq_len, d_model), lambda g, s: (0, 0, 0))
    gain = pl.BlockSpec((1, d_model), lambda g, s: (0, 0))
    in_w = pl.BlockSpec((per, d_model, head_dim), lambda g, s: (g, 0, 0))
    rows = n_seq * seq_len
    return pl.pallas_call(
        attention_kernel,
        out_shape=(out, out),
        grid=(n_heads // per, n_seq),
        in_specs=[gain, gain, pl.BlockSpec((1, n_seq, seq_len, d_model), lambda g, s: (micro, first // n_seq, 0, 0)), in_w, in_w, in_w, pl.BlockSpec((per, head_dim, d_model), lambda g, s: (g, 0, 0))],
        out_specs=(whole, whole),
        scratch_shapes=[pltpu.VMEM((n_seq, seq_len, d_model), jnp.bfloat16), pltpu.VMEM((n_seq, seq_len, d_model), jnp.float32)],
        compiler_params=pltpu.CompilerParams(dimension_semantics=("arbitrary", "arbitrary"), vmem_limit_bytes=VMEM_LIMIT),
        cost_estimate=pl.CostEstimate(flops=8 * rows * d_model * d_model, bytes_accessed=30_000_000, transcendentals=0),
        name="attention_rows",
    )(*gains, tokens, *weights)


def swiglu(in_rows, gate_w, up_w, down_w):
    gate_act = jnp.dot(in_rows, gate_w, preferred_element_type=jnp.float32)
    up_act = jnp.dot(in_rows, up_w, preferred_element_type=jnp.float32)
    hidden = (jax.nn.silu(gate_act) * up_act).astype(jnp.bfloat16)
    return jnp.dot(hidden, down_w, preferred_element_type=jnp.float32).astype(jnp.bfloat16)


def route_tables(local_ids, weights, n_local):
    n_src, _, n_tok = local_ids.shape
    hits = local_ids[:, :, None, :] == jnp.arange(n_local)[None, None, :, None]
    mask = jnp.any(hits, axis=1)
    upper = (jnp.arange(n_tok)[:, None] <= jnp.arange(n_tok)[None, :]).astype(jnp.bfloat16)
    running = jnp.dot(mask.astype(jnp.bfloat16).reshape(n_src * n_local, n_tok), upper, preferred_element_type=jnp.float32)
    running = running.astype(jnp.int32).reshape(n_src, n_local, n_tok)
    counts = running[:, :, -1]
    padded = (counts + SEG - 1) // SEG * SEG
    before_e = (jnp.arange(n_local)[:, None] < jnp.arange(n_local)[None, :]).astype(jnp.int32)
    before_s = (jnp.arange(n_src)[:, None] < jnp.arange(n_src)[None, :]).astype(jnp.int32)
    offs = jnp.sum(padded[:, :, None] * before_e[None], axis=1)
    places = jnp.sum(padded[:, None, :] * before_s[:, :, None], axis=0)
    slot_of = offs[:, :, None] + running - 1
    slots = jnp.sum(jnp.where(hits, slot_of[:, None] + 1, 0), axis=2) - 1
    table = jnp.concatenate([offs.reshape(-1), padded.reshape(-1), places.reshape(-1), jnp.sum(padded, axis=0), jnp.sum(padded, axis=1)])
    pad_rows = jnp.full((n_src, 8 - slots.shape[1], n_tok), -1, jnp.int32)
    slot_rows = jnp.concatenate([slots, pad_rows], axis=1)
    cols = jnp.concatenate([slots.astype(jnp.float32), weights], axis=1).transpose(0, 2, 1)
    return table, slot_rows, cols


def gather_kernel(n_src, n_local, top_count, table_ref, slots_ref, z_ref, x_hbm, buf, sems, sent):
    src = pl.program_id(0)
    n_tok = z_ref.shape[0]
    total = table_ref[3 * n_src * n_local + n_local + src]
    block = buf.shape[1]

    @pl.when(src == 0)
    def _():
        sent[0] = 0

    def copy(slot, row):
        return pltpu.make_async_copy(buf.at[slot], x_hbm.at[src, pl.ds(row, block)], sems.at[slot])

    def chunk(c, carry):
        base = pl.multiple_of(c * block, block)
        slot = sent[0] & 1

        @pl.when(sent[0] >= 2)
        def _():
            copy(slot, 0).wait()

        for part in range(block // ROWS):
            rows = lax.broadcasted_iota(jnp.int32, (ROWS, n_tok), 0) + (base + part * ROWS)
            hit = rows == slots_ref[0, 0:1, :]
            for j in range(1, top_count):
                hit = hit | (rows == slots_ref[0, j : j + 1, :])
            pick = jnp.where(hit, 1.0, 0.0).astype(jnp.bfloat16)
            got = jnp.dot(pick, z_ref[...], preferred_element_type=jnp.float32)
            buf[slot, part * ROWS : (part + 1) * ROWS, :] = got.astype(jnp.bfloat16)
        copy(slot, base).start()
        sent[0] = sent[0] + 1
        return carry

    lax.fori_loop(0, (total + block - 1) // block, chunk, 0)

    @pl.when(src == n_src - 1)
    def _():
        for back in (1, 2):

            @pl.when(sent[0] >= back)
            def _():
                copy((sent[0] - back) & 1, 0).wait()


def gather_rows(table, slot_rows, z_all, n_local, top_count, max_rows):
    n_src = slot_rows.shape[0]
    n_tok = z_all.shape[0] // n_src
    d_model = z_all.shape[1]
    block = 2 * ROWS
    return pl.pallas_call(
        functools.partial(gather_kernel, n_src, n_local, top_count),
        out_shape=jax.ShapeDtypeStruct((n_src, -(-max_rows // block) * block, d_model), jnp.bfloat16),
        grid_spec=pltpu.PrefetchScalarGridSpec(
            num_scalar_prefetch=1,
            grid=(n_src,),
            in_specs=[
                pl.BlockSpec((1, 8, n_tok), lambda s, t: (s, 0, 0)),
                pl.BlockSpec((n_tok, d_model), lambda s, t: (s, 0)),
            ],
            out_specs=pl.BlockSpec(memory_space=pl.ANY),
            scratch_shapes=[pltpu.VMEM((2, block, d_model), jnp.bfloat16), pltpu.SemaphoreType.DMA((2,)), pltpu.SMEM((1,), jnp.int32)],
        ),
        compiler_params=pltpu.CompilerParams(dimension_semantics=("arbitrary",), vmem_limit_bytes=VMEM_LIMIT),
        cost_estimate=pl.CostEstimate(flops=2 * 1024 * n_src * n_tok * d_model, bytes_accessed=6 * n_src * n_tok * d_model, transcendentals=0),
        name="gather_rows",
    )(table, slot_rows, z_all)


def expert_kernel(n_src, n_local, table_ref, x_hbm, ga, ua, da, gb, ub, db, y_hbm, x_buf, y_buf, in_sems, out_sems):
    step = pl.program_id(0)
    n_seg = n_src * n_local

    def pieces(which, act):
        slot = lax.rem(which, 2)
        for s in range(n_src):
            off = pl.multiple_of(table_ref[s * n_local + which], SEG)
            size = pl.multiple_of(table_ref[n_seg + s * n_local + which], SEG)
            place = pl.multiple_of(table_ref[2 * n_seg + s * n_local + which], SEG)
            act(slot, s, off, place, size)

    def in_copy(slot, s, off, place, size):
        return pltpu.make_async_copy(x_hbm.at[s, pl.ds(off, size)], x_buf.at[slot, pl.ds(place, size)], in_sems.at[slot, s])

    def out_copy(slot, s, off, place, size):
        return pltpu.make_async_copy(y_buf.at[slot, pl.ds(place, size)], y_hbm.at[s, pl.ds(off, size)], out_sems.at[slot, s])

    @pl.when(step == 0)
    def _():
        pieces(step, lambda *a: in_copy(*a).start())

    @pl.when(step + 1 < n_local)
    def _():
        pieces(step + 1, lambda *a: in_copy(*a).start())

    pieces(step, lambda *a: in_copy(*a).wait())

    @pl.when(step >= 2)
    def _():
        pieces(step - 2, lambda *a: out_copy(*a).wait())

    slot = lax.rem(step, 2)
    total = table_ref[3 * n_seg + step]
    n_blocks = (total + ROWS - 1) // ROWS

    def run(gate, up, down):
        def block(c, carry):
            rows = pl.ds(pl.multiple_of(c * ROWS, ROWS), ROWS)
            x = x_buf[slot, rows, :]
            g = jnp.dot(x, gate[0], preferred_element_type=jnp.float32)
            u = jnp.dot(x, up[0], preferred_element_type=jnp.float32)
            h = (g * jax.nn.sigmoid(g) * u).astype(jnp.bfloat16)
            y_buf[slot, rows, :] = jnp.dot(h, down[0], preferred_element_type=jnp.float32).astype(jnp.bfloat16)
            return carry

        lax.fori_loop(0, n_blocks, block, 0)

    @pl.when(step < n_local // 2)
    def _():
        run(ga, ua, da)

    @pl.when(step >= n_local // 2)
    def _():
        run(gb, ub, db)

    pieces(step, lambda *a: out_copy(*a).start())

    @pl.when(step == n_local - 1)
    def _():
        pieces(step - 1, lambda *a: out_copy(*a).wait())
        pieces(step, lambda *a: out_copy(*a).wait())


def expert_rows(table, x_rows, own, other, buf_rows):
    n_src, _, d_model = x_rows.shape
    half, _, width = own[0].shape
    n_local = 2 * half
    own_at = lambda l, t: (jnp.minimum(l, half - 1), 0, 0)
    other_at = lambda l, t: (jnp.maximum(l - half, 0), 0, 0)
    return pl.pallas_call(
        functools.partial(expert_kernel, n_src, n_local),
        out_shape=jax.ShapeDtypeStruct(x_rows.shape, jnp.bfloat16),
        grid_spec=pltpu.PrefetchScalarGridSpec(
            num_scalar_prefetch=1,
            grid=(n_local,),
            in_specs=[
                pl.BlockSpec(memory_space=pl.ANY),
                pl.BlockSpec((1, d_model, width), own_at),
                pl.BlockSpec((1, d_model, width), own_at),
                pl.BlockSpec((1, width, d_model), own_at),
                pl.BlockSpec((1, d_model, width), other_at),
                pl.BlockSpec((1, d_model, width), other_at),
                pl.BlockSpec((1, width, d_model), other_at),
            ],
            out_specs=pl.BlockSpec(memory_space=pl.ANY),
            scratch_shapes=[
                pltpu.VMEM((2, buf_rows, d_model), jnp.bfloat16),
                pltpu.VMEM((2, buf_rows, d_model), jnp.bfloat16),
                pltpu.SemaphoreType.DMA((2, n_src)),
                pltpu.SemaphoreType.DMA((2, n_src)),
            ],
        ),
        compiler_params=pltpu.CompilerParams(dimension_semantics=("arbitrary",), vmem_limit_bytes=VMEM_LIMIT),
        cost_estimate=pl.CostEstimate(flops=2 * 8192 * d_model * width * 3, bytes_accessed=115_000_000, transcendentals=0),
        name="expert_rows",
    )(table, x_rows, *own, *other)


def combine_kernel(n_src, n_local, top_count, table_ref, cols_ref, y_hbm, out_ref, slot_bc, weight_bc, buf, sems):
    src = pl.program_id(0)
    n_tok = out_ref.shape[0]
    at_total = 3 * n_src * n_local + n_local
    total = table_ref[at_total + src]
    n_chunks = (total + ROWS - 1) // ROWS
    lanes = 128
    ahead = 2 + (src & 1)

    def copy(which, c, slot):
        return pltpu.make_async_copy(y_hbm.at[which, pl.ds(pl.multiple_of(c * ROWS, ROWS), ROWS)], buf.at[slot], sems.at[slot])

    @pl.when(src == 0)
    def _():
        copy(src, 0, ahead).start()

    @pl.when(src + 1 < n_src)
    def _():
        copy(src + 1, 0, 5 - ahead).start()

    @pl.when(n_chunks > 1)
    def _():
        copy(src, 1, 1).start()

    for j in range(top_count):
        slot_bc[j] = jnp.broadcast_to(cols_ref[0, :, j : j + 1], (n_tok, lanes))
        weight_bc[j] = jnp.broadcast_to(cols_ref[0, :, top_count + j : top_count + j + 1], (n_tok, lanes))
    out_ref[...] = jnp.zeros_like(out_ref)
    copy(src, 0, ahead).wait()

    def chunk(c, carry):
        base = c * ROWS
        slot = jnp.where(c == 0, ahead, c & 1)

        @pl.when(c > 0)
        def _():
            copy(src, c, slot).wait()

        @pl.when((c > 0) & (c + 1 < n_chunks))
        def _():
            copy(src, c + 1, (c + 1) & 1).start()

        y = buf[slot]
        y_at = lax.broadcasted_iota(jnp.int32, y.shape, 0) + base
        y = jnp.where(y_at < total, y, jnp.zeros_like(y))
        for i in range(n_tok // ROWS):
            tok = slice(i * ROWS, (i + 1) * ROWS)
            parts = [[], [], []]
            for half in range(ROWS // lanes):
                lane_at = (lax.broadcasted_iota(jnp.int32, (ROWS, lanes), 1) + (base + half * lanes)).astype(jnp.float32)
                coef = jnp.zeros((ROWS, lanes), jnp.float32)
                for j in range(top_count):
                    coef = jnp.where(slot_bc[j, tok, :] == lane_at, weight_bc[j, tok, :], coef)
                high = coef.astype(jnp.bfloat16)
                rest = coef - high.astype(jnp.float32)
                mid = rest.astype(jnp.bfloat16)
                low = (rest - mid.astype(jnp.float32)).astype(jnp.bfloat16)
                for part, val in zip(parts, (high, mid, low)):
                    part.append(val)
            high, mid, low = (jnp.concatenate(part, axis=1) for part in parts)
            acc = jnp.dot(low, y, preferred_element_type=jnp.float32)
            acc = acc + jnp.dot(mid, y, preferred_element_type=jnp.float32)
            acc = acc + jnp.dot(high, y, preferred_element_type=jnp.float32)
            out_ref[tok, :] += acc
        return carry

    lax.fori_loop(0, n_chunks, chunk, 0)


def combine_rows(table, cols, y_rows, n_local, top_count):
    n_src, _, d_model = y_rows.shape
    n_tok = cols.shape[1]
    return pl.pallas_call(
        functools.partial(combine_kernel, n_src, n_local, top_count),
        out_shape=jax.ShapeDtypeStruct((n_src * n_tok, d_model), jnp.float32),
        grid_spec=pltpu.PrefetchScalarGridSpec(
            num_scalar_prefetch=1,
            grid=(n_src,),
            in_specs=[
                pl.BlockSpec((1, n_tok, 2 * top_count), lambda s, t: (s, 0, 0)),
                pl.BlockSpec(memory_space=pl.ANY),
            ],
            out_specs=pl.BlockSpec((n_tok, d_model), lambda s, t: (s, 0)),
            scratch_shapes=[
                pltpu.VMEM((top_count, n_tok, 128), jnp.float32),
                pltpu.VMEM((top_count, n_tok, 128), jnp.float32),
                pltpu.VMEM((4, ROWS, d_model), jnp.bfloat16),
                pltpu.SemaphoreType.DMA((4,)),
            ],
        ),
        compiler_params=pltpu.CompilerParams(dimension_semantics=("arbitrary",), vmem_limit_bytes=VMEM_LIMIT),
        cost_estimate=pl.CostEstimate(flops=6 * 1024 * n_src * n_tok * d_model, bytes_accessed=8 * n_src * n_tok * d_model, transcendentals=0),
        name="combine_rows",
    )(table, cols, y_rows)


def unit_list(n_micro, n_seq):
    units = [(0, q, 1) for q in range(n_seq)]
    return units + [(micro, 0, n_seq) for micro in range(1, n_micro)]


def solution(mesh):
    group_size = mesh.shape["ep"]
    n_src = group_size // 2
    ring_groups = [[2 * k + core for k in range(n_src)] for core in range(2)]
    pair_perm = [(k, k ^ 1) for k in range(group_size)]

    def device_step(tokens, expert_ids, route_weights, attn_norm, w_query, w_key, w_value, w_out, ffn_norm, w_gate, w_up, w_down, shared_gate, shared_up, shared_down):
        n_micro, n_seq, seq_len, d_model = tokens.shape
        n_tok = n_seq * seq_len
        top_count = expert_ids.shape[-1]
        half = w_gate.shape[0]
        n_local = 2 * half
        slot_cap = capacity_of(n_tok, top_count, half * group_size)
        max_rows = n_local * slot_cap
        me = lax.axis_index("ep")

        own = (w_gate, w_up, w_down)
        other = tuple(lax.ppermute(w, "ep", pair_perm) for w in own)

        meta = jnp.concatenate([expert_ids.astype(jnp.float32).transpose(0, 2, 1), route_weights.transpose(0, 2, 1), jnp.zeros((n_micro, 16 - 2 * top_count, n_tok), jnp.float32)], axis=1)
        meta = lax.all_gather(meta.reshape(n_micro * 16, n_tok), "ep", axis=0, tiled=True)
        meta = meta.reshape(n_src, 2, n_micro, 16, n_tok)
        meta = lax.dynamic_index_in_dim(meta, me % 2, axis=1, keepdims=False)
        ids = meta[:, :, :top_count].astype(jnp.int32)
        all_weights = meta[:, :, top_count : 2 * top_count]
        from_own = ids - half * me
        from_other = ids - half * (me ^ 1)
        local_ids = jnp.where((from_own >= 0) & (from_own < half), from_own, jnp.where((from_other >= 0) & (from_other < half), from_other + half, -1))

        gains = (attn_norm.reshape(1, d_model), ffn_norm.reshape(1, d_model))
        attn_weights = (w_query.transpose(1, 0, 2), w_key.transpose(1, 0, 2), w_value.transpose(1, 0, 2), w_out)
        units = unit_list(n_micro, n_seq)
        hs, zs, gathered, plans = [], [], [], []
        for micro, first, count in units:
            if zs:
                tokens, _ = lax.optimization_barrier((tokens, zs[-1]))
            h, z = attention_rows(tokens, micro, first, count, gains, attn_weights)
            h, z = (v.reshape(count * seq_len, d_model) for v in (h, z))
            hs.append(h)
            zs.append(z)
            gathered.append(lax.all_gather(z, "ep", axis=0, tiled=True, axis_index_groups=ring_groups))
            by_seq = lambda v: v[:, micro].reshape(n_src, top_count, n_seq, seq_len)[:, :, first : first + count].transpose(0, 2, 1, 3).reshape(n_src * count, top_count, seq_len)
            plans.append(route_tables(by_seq(local_ids), by_seq(all_weights), n_local))
        routed, partial = [], None
        for k, (table, slot_rows, cols) in enumerate(plans):
            if partial is not None:
                table, _ = lax.optimization_barrier((table, partial))
            x_rows = gather_rows(table, slot_rows, gathered[k], n_local, top_count, max_rows)
            seg_rows = min(slot_cap, seq_len) * n_src * units[k][2] if units[k][2] == 1 else (slot_cap + SEG * units[k][2]) * n_src
            y_rows = expert_rows(table, x_rows, own, other, -(-seg_rows // ROWS) * ROWS)
            partial = combine_rows(table, cols, y_rows, n_local, top_count)
            routed.append(lax.psum_scatter(partial, "ep", scatter_dimension=0, tiled=True, axis_index_groups=ring_groups))
        outs = [[] for _ in range(n_micro)]
        for k, (micro, first, count) in enumerate(units):
            z = zs[k]
            shared_out = swiglu(z, shared_gate, shared_up, shared_down)
            layer_rows = hs[k].astype(jnp.float32) + shared_out.astype(jnp.float32) + routed[k]
            outs[micro].append(layer_rows.astype(jnp.bfloat16).reshape(count, seq_len, d_model))
        return jnp.stack([jnp.concatenate(parts, axis=0) if len(parts) > 1 else parts[0] for parts in outs])

    token_spec = P(None, ("dp", "ep"), None, None)
    route_spec = P(None, ("dp", "ep"), None)
    rep_spec = P()
    expert_spec = P("ep", None, None)
    in_specs = (token_spec, route_spec, route_spec, rep_spec, rep_spec, rep_spec, rep_spec, rep_spec, rep_spec, expert_spec, expert_spec, expert_spec, rep_spec, rep_spec, rep_spec)

    return jax.shard_map(device_step, mesh=mesh, in_specs=in_specs, out_specs=token_spec, check_vma=False)
```

```python
import functools

import jax
import jax.numpy as jnp
from jax import lax
from jax.experimental import pallas as pl
from jax.experimental.pallas import tpu as pltpu
from jax.sharding import PartitionSpec as P


NORM_EPS = 1e-6
CAP_FACTOR = 2
SLOT_ALIGN = 8
SEG = 16
ROWS = 256
Q_BLOCKS = 1
FIELD = 128
PIECE = 8 * FIELD
BY_HOPS = True
VMEM_LIMIT = 64_000_000


def capacity_of(n_tok, top_count, experts):
    return SLOT_ALIGN * ((CAP_FACTOR * n_tok * top_count + SLOT_ALIGN * experts - 1) // (SLOT_ALIGN * experts))


def rms_norm(in_vals, norm_gain):
    wide_vals = in_vals.astype(jnp.float32)
    inv_rms = lax.rsqrt(jnp.mean(wide_vals * wide_vals, axis=-1, keepdims=True) + NORM_EPS)
    return (wide_vals * inv_rms * norm_gain.astype(jnp.float32)).astype(jnp.bfloat16)


def attention_kernel(gain_ref, ffn_gain_ref, x_ref, wq_ref, wk_ref, wv_ref, wo_ref, h_ref, z_ref, normed, acc):
    group, seq = pl.program_id(0), pl.program_id(1)
    seq_len, d_model = normed.shape[1:]
    per, _, head_dim = wq_ref.shape
    block = seq_len // Q_BLOCKS

    @pl.when(group == 0)
    def _():
        normed[seq] = rms_norm(x_ref[0, seq], gain_ref[...])

    rows = normed[seq]
    project = lambda w_ref: jnp.dot(rows, jnp.concatenate([w_ref[i] for i in range(per)], axis=1), preferred_element_type=jnp.float32).astype(jnp.bfloat16)
    queries, key_rows, value_rows = project(wq_ref), project(wk_ref), project(wv_ref)
    above = lax.broadcasted_iota(jnp.int32, (block, block), 0) < lax.broadcasted_iota(jnp.int32, (block, block), 1)
    heads = []
    for i in range(per):
        lanes = slice(i * head_dim, (i + 1) * head_dim)
        k, v = key_rows[:, lanes], value_rows[:, lanes]
        outs = []
        for part in range(Q_BLOCKS):
            q = queries[part * block : (part + 1) * block, lanes]
            scores = lax.dot_general(q, k[: (part + 1) * block], (((1,), (1,)), ((), ())), preferred_element_type=jnp.float32) * (head_dim**-0.5)
            diag = jnp.where(above, -jnp.inf, scores[:, part * block :])
            scores = diag if part == 0 else jnp.concatenate([scores[:, : part * block], diag], axis=1)
            shifted = jnp.exp(scores - jnp.max(scores, axis=1, keepdims=True))
            probs = (shifted * (1.0 / jnp.sum(shifted, axis=1, keepdims=True))).astype(jnp.bfloat16)
            outs.append(jnp.dot(probs, v[: (part + 1) * block], preferred_element_type=jnp.float32).astype(jnp.bfloat16))
        heads.append(jnp.concatenate(outs, axis=0))
    mix = jnp.concatenate(heads, axis=1)
    added = jnp.dot(mix, wo_ref[...].reshape(per * head_dim, d_model), preferred_element_type=jnp.float32)

    @pl.when(group == 0)
    def _():
        acc[seq] = added

    @pl.when(group > 0)
    def _():
        acc[seq] += added

    @pl.when(group == pl.num_programs(0) - 1)
    def _():
        residual = (x_ref[0, seq].astype(jnp.float32) + acc[seq]).astype(jnp.bfloat16)
        h_ref[seq] = residual
        z_ref[seq] = rms_norm(residual, ffn_gain_ref[...])


def attention_rows(tokens, micro, first, n_seq, gains, weights):
    _, _, seq_len, d_model = tokens.shape
    n_heads, _, head_dim = weights[0].shape
    per = 4 if n_heads % 4 == 0 else 1
    out = jax.ShapeDtypeStruct((n_seq, seq_len, d_model), jnp.bfloat16)
    whole = pl.BlockSpec((n_seq, seq_len, d_model), lambda g, s: (0, 0, 0))
    gain = pl.BlockSpec((1, d_model), lambda g, s: (0, 0))
    in_w = pl.BlockSpec((per, d_model, head_dim), lambda g, s: (g, 0, 0))
    rows = n_seq * seq_len
    return pl.pallas_call(
        attention_kernel,
        out_shape=(out, out),
        grid=(n_heads // per, n_seq),
        in_specs=[gain, gain, pl.BlockSpec((1, n_seq, seq_len, d_model), lambda g, s: (micro, first // n_seq, 0, 0)), in_w, in_w, in_w, pl.BlockSpec((per, head_dim, d_model), lambda g, s: (g, 0, 0))],
        out_specs=(whole, whole),
        scratch_shapes=[pltpu.VMEM((n_seq, seq_len, d_model), jnp.bfloat16), pltpu.VMEM((n_seq, seq_len, d_model), jnp.float32)],
        compiler_params=pltpu.CompilerParams(dimension_semantics=("arbitrary", "arbitrary"), vmem_limit_bytes=VMEM_LIMIT),
        cost_estimate=pl.CostEstimate(flops=8 * rows * d_model * d_model, bytes_accessed=30_000_000, transcendentals=0),
        name="attention_rows",
    )(*gains, tokens, *weights)


def swiglu(in_rows, gate_w, up_w, down_w):
    gate_act = jnp.dot(in_rows, gate_w, preferred_element_type=jnp.float32)
    up_act = jnp.dot(in_rows, up_w, preferred_element_type=jnp.float32)
    hidden = (jax.nn.silu(gate_act) * up_act).astype(jnp.bfloat16)
    return jnp.dot(hidden, down_w, preferred_element_type=jnp.float32).astype(jnp.bfloat16)


def route_kernel(half, top_count, me_ref, meta_ref, slots_ref, cols_ref, table_ref, upper, placed):
    micro, src, seq = (pl.program_id(i) for i in range(3))
    me = me_ref[0]
    n_local, n_tok = 2 * half, upper.shape[0]
    acc = jnp.where(micro == 0, seq, 0)

    @pl.when((micro == 0) & (src == 0) & (seq == 0))
    def _():
        below = lax.broadcasted_iota(jnp.int32, upper.shape, 0) <= lax.broadcasted_iota(jnp.int32, upper.shape, 1)
        upper[...] = jnp.where(below, 1.0, 0.0).astype(jnp.bfloat16)

    @pl.when((src == 0) & ((micro == 0) | (seq == 0)))
    def _():
        placed[acc] = jnp.zeros(placed.shape[1:], jnp.float32)

    ids = meta_ref[0:top_count, :].astype(jnp.int32)
    from_own, from_other = ids - half * me, ids - half * (me ^ 1)
    local = jnp.where((from_own >= 0) & (from_own < half), from_own, jnp.where((from_other >= 0) & (from_other < half), from_other + half, -1))
    expert_at = lax.broadcasted_iota(jnp.int32, (n_local, n_tok), 0)
    hits = [local[j : j + 1, :] == expert_at for j in range(top_count)]
    mask = jnp.where(functools.reduce(jnp.logical_or, hits), 1.0, 0.0)
    bits = mask.astype(jnp.bfloat16)
    running = jnp.dot(bits, upper[...], preferred_element_type=jnp.float32)
    pad = lambda counts: jnp.floor((counts + (SEG - 1)) * (1.0 / SEG))
    units = jnp.broadcast_to(pad(running[:, n_tok - 1 : n_tok]), (n_local, FIELD)).astype(jnp.bfloat16)
    before = lax.broadcasted_iota(jnp.int32, (n_local, n_local), 1) < lax.broadcasted_iota(jnp.int32, (n_local, n_local), 0)
    offs = jnp.dot(jnp.where(before, 1.0, 0.0).astype(jnp.bfloat16), units, preferred_element_type=jnp.float32) * SEG
    row_of = offs[:, 0:1] + running
    slots = [jnp.sum(jnp.where(hit, row_of, 0.0), axis=0, keepdims=True) - 1.0 for hit in hits]
    none = jnp.full((1, n_tok), -1.0, jnp.float32)
    slots_ref[...] = jnp.concatenate(slots + [none] * (8 - top_count), axis=0).astype(jnp.int32)
    cols_ref[...] = jnp.concatenate(slots + [meta_ref[top_count : 2 * top_count, :]] + [none] * (16 - 2 * top_count), axis=0)
    wide = jnp.concatenate([bits, jnp.zeros((FIELD - n_local, n_tok), jnp.bfloat16)], axis=0)
    counts = lax.dot_general(jnp.ones((8, n_tok), jnp.bfloat16), wide, (((1,), (1,)), ((), ())), preferred_element_type=jnp.float32)
    units_row = pad(counts)
    before_row = lax.broadcasted_iota(jnp.int32, (FIELD, FIELD), 0) < lax.broadcasted_iota(jnp.int32, (FIELD, FIELD), 1)
    offs_row = jnp.dot(units_row.astype(jnp.bfloat16), jnp.where(before_row, 1.0, 0.0).astype(jnp.bfloat16), preferred_element_type=jnp.float32) * SEG
    sizes_row = units_row * SEG
    at = lax.broadcasted_iota(jnp.int32, (8, FIELD), 0)
    fields = jnp.where(at == 0, offs_row, jnp.where(at == 1, sizes_row, placed[acc]))
    table_ref[...] = fields.astype(jnp.int32)
    placed[acc] = placed[acc] + sizes_row


def route_rows(meta, me, half, top_count, n_src, n_micro, n_seq, seq_len):
    spot = lambda m, s, q, t: (m, s, q, 0, 0)
    piece = lambda rows, lanes, dtype: (jax.ShapeDtypeStruct((n_micro, n_src, n_seq, rows, lanes), dtype), pl.BlockSpec((None, None, None, rows, lanes), spot))
    outs = [piece(8, seq_len, jnp.int32), piece(16, seq_len, jnp.float32), piece(8, FIELD, jnp.int32)]
    return pl.pallas_call(
        functools.partial(route_kernel, half, top_count),
        out_shape=tuple(o[0] for o in outs),
        grid_spec=pltpu.PrefetchScalarGridSpec(
            num_scalar_prefetch=1,
            grid=(n_micro, n_src, n_seq),
            in_specs=[pl.BlockSpec((16, seq_len), lambda m, s, q, t: ((2 * s + lax.rem(t[0], 2)) * n_micro + m, q))],
            out_specs=tuple(o[1] for o in outs),
            scratch_shapes=[pltpu.VMEM((seq_len, seq_len), jnp.bfloat16), pltpu.VMEM((n_seq, 8, FIELD), jnp.float32)],
        ),
        compiler_params=pltpu.CompilerParams(dimension_semantics=("arbitrary",) * 3),
        cost_estimate=pl.CostEstimate(flops=500_000_000, bytes_accessed=2_000_000, transcendentals=0),
        name="route_rows",
    )(me, meta)


class Unit:
    def __init__(self, micro, first, count, n_src, n_seq):
        self.micro, self.first, self.count, self.n_src, self.n_seq = micro, first, count, n_src, n_seq
        self.pieces = n_src * count

    def spot(self, i):
        return self.micro, i // self.count, self.first + i % self.count

    def field(self, table_ref, i, which, expert):
        micro, src, seq = self.spot(i)
        return table_ref[((micro * self.n_src + src) * self.n_seq + seq) * PIECE + which * FIELD + expert]

    def rows_of(self, table_ref, i, n_local):
        return self.field(table_ref, i, 0, n_local - 1) + self.field(table_ref, i, 1, n_local - 1)

    def spec(self, rows, lanes):
        return pl.BlockSpec((None, None, None, rows, lanes), lambda i, *_: (*self.spot(i), 0, 0))


def gather_kernel(unit, n_local, top_count, table_ref, slots_ref, *refs):
    z_refs, (x_hbm, buf, sems, sent) = refs[: -4 if len(refs) == 5 else -6], (refs[-4:] if len(refs) == 5 else refs[-6:-2])
    src = pl.program_id(0)
    total = unit.rows_of(table_ref, src, n_local)
    block = buf.shape[1]
    n_tok = slots_ref.shape[1]
    if len(refs) == 5:
        z = z_refs[0]
    else:
        z_buf, z_sems = refs[-2:]
        x_at = table_ref[table_ref.shape[0] - 1] // 2

        def fetch(i):
            _, s, q = unit.spot(i)
            away = lax.rem(s - x_at + unit.n_src, unit.n_src)
            own, left, right, far = z_refs[0], z_refs[1:3], z_refs[3:5], z_refs[5:7]
            for seq in range(unit.count):
                for hop, ref in enumerate((own.at[seq], right[seq], far[seq], left[seq])):

                    @pl.when((q == seq) & (away == hop))
                    def _():
                        pltpu.make_async_copy(ref, z_buf.at[i & 1], z_sems.at[i & 1]).start()

        @pl.when(src == 0)
        def _():
            fetch(src)

        @pl.when(src + 1 < unit.pieces)
        def _():
            fetch(src + 1)

        pltpu.make_async_copy(z_refs[1], z_buf.at[src & 1], z_sems.at[src & 1]).wait()
        z = z_buf.at[src & 1]

    @pl.when(src == 0)
    def _():
        sent[0] = 0

    def copy(slot, row):
        return pltpu.make_async_copy(buf.at[slot], x_hbm.at[src, pl.ds(row, block)], sems.at[slot])

    def chunk(c, carry):
        base = pl.multiple_of(c * block, block)
        slot = sent[0] & 1

        @pl.when(sent[0] >= 2)
        def _():
            copy(slot, 0).wait()

        for part in range(block // ROWS):
            rows = lax.broadcasted_iota(jnp.int32, (ROWS, n_tok), 0) + (base + part * ROWS)
            hit = rows == slots_ref[0:1, :]
            for j in range(1, top_count):
                hit = hit | (rows == slots_ref[j : j + 1, :])
            pick = jnp.where(hit, 1.0, 0.0).astype(jnp.bfloat16)
            got = jnp.dot(pick, z[...], preferred_element_type=jnp.float32)
            buf[slot, part * ROWS : (part + 1) * ROWS, :] = got.astype(jnp.bfloat16)
        copy(slot, base).start()
        sent[0] = sent[0] + 1
        return carry

    lax.fori_loop(0, (total + block - 1) // block, chunk, 0)

    @pl.when(src == unit.pieces - 1)
    def _():
        for back in (1, 2):

            @pl.when(sent[0] >= back)
            def _():
                copy((sent[0] - back) & 1, 0).wait()


def gather_rows(unit, table, slots, zs, n_local, top_count, max_rows):
    n_tok = slots.shape[-1]
    d_model = zs[0].shape[-1]
    block = 2 * ROWS
    held = len(zs) > 1
    z_specs = [pl.BlockSpec(memory_space=pl.ANY)] * len(zs) if held else [pl.BlockSpec((n_tok, d_model), lambda i, t: (i, 0))]
    scratch = [pltpu.VMEM((2, block, d_model), jnp.bfloat16), pltpu.SemaphoreType.DMA((2,)), pltpu.SMEM((1,), jnp.int32)]
    if held:
        scratch += [pltpu.VMEM((2, n_tok, d_model), jnp.bfloat16), pltpu.SemaphoreType.DMA((2,))]
    return pl.pallas_call(
        functools.partial(gather_kernel, unit, n_local, top_count),
        out_shape=jax.ShapeDtypeStruct((unit.pieces, -(-max_rows // block) * block, d_model), jnp.bfloat16),
        grid_spec=pltpu.PrefetchScalarGridSpec(
            num_scalar_prefetch=1,
            grid=(unit.pieces,),
            in_specs=[unit.spec(8, n_tok), *z_specs],
            out_specs=pl.BlockSpec(memory_space=pl.ANY),
            scratch_shapes=scratch,
        ),
        compiler_params=pltpu.CompilerParams(dimension_semantics=("arbitrary",), vmem_limit_bytes=VMEM_LIMIT),
        cost_estimate=pl.CostEstimate(flops=2 * 1024 * unit.pieces * n_tok * d_model, bytes_accessed=6 * unit.pieces * n_tok * d_model, transcendentals=0),
        name="gather_rows",
    )(table, slots, *zs)


def expert_kernel(unit, n_local, table_ref, x_hbm, ga, ua, da, gb, ub, db, y_hbm, x_buf, y_buf, in_sems, out_sems):
    step = pl.program_id(0)

    def pieces(which, act):
        slot = lax.rem(which, 2)
        for s in range(unit.pieces):
            off, size, place = (pl.multiple_of(unit.field(table_ref, s, f, which), SEG) for f in range(3))
            act(slot, s, off, place, size)

    def in_copy(slot, s, off, place, size):
        return pltpu.make_async_copy(x_hbm.at[s, pl.ds(off, size)], x_buf.at[slot, pl.ds(place, size)], in_sems.at[slot, s])

    def out_copy(slot, s, off, place, size):
        return pltpu.make_async_copy(y_buf.at[slot, pl.ds(place, size)], y_hbm.at[s, pl.ds(off, size)], out_sems.at[slot, s])

    @pl.when(step == 0)
    def _():
        pieces(step, lambda *a: in_copy(*a).start())

    @pl.when(step + 1 < n_local)
    def _():
        pieces(step + 1, lambda *a: in_copy(*a).start())

    pieces(step, lambda *a: in_copy(*a).wait())

    @pl.when(step >= 2)
    def _():
        pieces(step - 2, lambda *a: out_copy(*a).wait())

    slot = lax.rem(step, 2)
    total = unit.field(table_ref, unit.pieces - 1, 1, step) + unit.field(table_ref, unit.pieces - 1, 2, step)
    n_blocks = (total + ROWS - 1) // ROWS

    def run(gate, up, down):
        def block(c, carry):
            rows = pl.ds(pl.multiple_of(c * ROWS, ROWS), ROWS)
            x = x_buf[slot, rows, :]
            g = jnp.dot(x, gate[0], preferred_element_type=jnp.float32)
            u = jnp.dot(x, up[0], preferred_element_type=jnp.float32)
            h = (g * jax.nn.sigmoid(g) * u).astype(jnp.bfloat16)
            y_buf[slot, rows, :] = jnp.dot(h, down[0], preferred_element_type=jnp.float32).astype(jnp.bfloat16)
            return carry

        lax.fori_loop(0, n_blocks, block, 0)

    @pl.when(step < n_local // 2)
    def _():
        run(ga, ua, da)

    @pl.when(step >= n_local // 2)
    def _():
        run(gb, ub, db)

    pieces(step, lambda *a: out_copy(*a).start())

    @pl.when(step == n_local - 1)
    def _():
        pieces(step - 1, lambda *a: out_copy(*a).wait())
        pieces(step, lambda *a: out_copy(*a).wait())


def expert_rows(unit, table, x_rows, own, other, buf_rows):
    n_src, _, d_model = x_rows.shape
    half, _, width = own[0].shape
    n_local = 2 * half
    own_at = lambda l, t: (jnp.minimum(l, half - 1), 0, 0)
    other_at = lambda l, t: (jnp.maximum(l - half, 0), 0, 0)
    return pl.pallas_call(
        functools.partial(expert_kernel, unit, n_local),
        out_shape=jax.ShapeDtypeStruct(x_rows.shape, jnp.bfloat16),
        grid_spec=pltpu.PrefetchScalarGridSpec(
            num_scalar_prefetch=1,
            grid=(n_local,),
            in_specs=[
                pl.BlockSpec(memory_space=pl.ANY),
                pl.BlockSpec((1, d_model, width), own_at),
                pl.BlockSpec((1, d_model, width), own_at),
                pl.BlockSpec((1, width, d_model), own_at),
                pl.BlockSpec((1, d_model, width), other_at),
                pl.BlockSpec((1, d_model, width), other_at),
                pl.BlockSpec((1, width, d_model), other_at),
            ],
            out_specs=pl.BlockSpec(memory_space=pl.ANY),
            scratch_shapes=[
                pltpu.VMEM((2, buf_rows, d_model), jnp.bfloat16),
                pltpu.VMEM((2, buf_rows, d_model), jnp.bfloat16),
                pltpu.SemaphoreType.DMA((2, n_src)),
                pltpu.SemaphoreType.DMA((2, n_src)),
            ],
        ),
        compiler_params=pltpu.CompilerParams(dimension_semantics=("arbitrary",), vmem_limit_bytes=VMEM_LIMIT),
        cost_estimate=pl.CostEstimate(flops=2 * 8192 * d_model * width * 3, bytes_accessed=115_000_000, transcendentals=0),
        name="expert_rows",
    )(table, x_rows, *own, *other)


def combine_kernel(unit, n_local, top_count, table_ref, cols_ref, y_hbm, out_ref, slot_bc, weight_bc, buf, sems):
    src = pl.program_id(0)
    n_tok = out_ref.shape[0]
    n_src = unit.pieces
    total = unit.rows_of(table_ref, src, n_local)
    n_chunks = (total + ROWS - 1) // ROWS
    lanes = 128
    ahead = 2 + (src & 1)

    def copy(which, c, slot):
        return pltpu.make_async_copy(y_hbm.at[which, pl.ds(pl.multiple_of(c * ROWS, ROWS), ROWS)], buf.at[slot], sems.at[slot])

    @pl.when(src == 0)
    def _():
        copy(src, 0, ahead).start()

    @pl.when(src + 1 < n_src)
    def _():
        copy(src + 1, 0, 5 - ahead).start()

    @pl.when(n_chunks > 1)
    def _():
        copy(src, 1, 1).start()

    cols = cols_ref[...].T
    for j in range(top_count):
        slot_bc[j] = jnp.broadcast_to(cols[:, j : j + 1], (n_tok, lanes))
        weight_bc[j] = jnp.broadcast_to(cols[:, top_count + j : top_count + j + 1], (n_tok, lanes))
    out_ref[...] = jnp.zeros_like(out_ref)
    copy(src, 0, ahead).wait()

    def chunk(c, carry):
        base = c * ROWS
        slot = jnp.where(c == 0, ahead, c & 1)

        @pl.when(c > 0)
        def _():
            copy(src, c, slot).wait()

        @pl.when((c > 0) & (c + 1 < n_chunks))
        def _():
            copy(src, c + 1, (c + 1) & 1).start()

        y = buf[slot]
        y_at = lax.broadcasted_iota(jnp.int32, y.shape, 0) + base
        y = jnp.where(y_at < total, y, jnp.zeros_like(y))
        for i in range(n_tok // ROWS):
            tok = slice(i * ROWS, (i + 1) * ROWS)
            parts = [[], [], []]
            for half in range(ROWS // lanes):
                lane_at = (lax.broadcasted_iota(jnp.int32, (ROWS, lanes), 1) + (base + half * lanes)).astype(jnp.float32)
                coef = jnp.zeros((ROWS, lanes), jnp.float32)
                for j in range(top_count):
                    coef = jnp.where(slot_bc[j, tok, :] == lane_at, weight_bc[j, tok, :], coef)
                high = coef.astype(jnp.bfloat16)
                rest = coef - high.astype(jnp.float32)
                mid = rest.astype(jnp.bfloat16)
                low = (rest - mid.astype(jnp.float32)).astype(jnp.bfloat16)
                for part, val in zip(parts, (high, mid, low)):
                    part.append(val)
            high, mid, low = (jnp.concatenate(part, axis=1) for part in parts)
            acc = jnp.dot(low, y, preferred_element_type=jnp.float32)
            acc = acc + jnp.dot(mid, y, preferred_element_type=jnp.float32)
            acc = acc + jnp.dot(high, y, preferred_element_type=jnp.float32)
            out_ref[tok, :] += acc
        return carry

    lax.fori_loop(0, n_chunks, chunk, 0)


def combine_rows(unit, table, cols, y_rows, n_local, top_count):
    n_src, _, d_model = y_rows.shape
    n_tok = cols.shape[-1]
    return pl.pallas_call(
        functools.partial(combine_kernel, unit, n_local, top_count),
        out_shape=jax.ShapeDtypeStruct((n_src * n_tok, d_model), jnp.float32),
        grid_spec=pltpu.PrefetchScalarGridSpec(
            num_scalar_prefetch=1,
            grid=(n_src,),
            in_specs=[
                unit.spec(16, n_tok),
                pl.BlockSpec(memory_space=pl.ANY),
            ],
            out_specs=pl.BlockSpec((n_tok, d_model), lambda s, t: (s, 0)),
            scratch_shapes=[
                pltpu.VMEM((top_count, n_tok, 128), jnp.float32),
                pltpu.VMEM((top_count, n_tok, 128), jnp.float32),
                pltpu.VMEM((4, ROWS, d_model), jnp.bfloat16),
                pltpu.SemaphoreType.DMA((4,)),
            ],
        ),
        compiler_params=pltpu.CompilerParams(dimension_semantics=("arbitrary",), vmem_limit_bytes=VMEM_LIMIT),
        cost_estimate=pl.CostEstimate(flops=6 * 1024 * n_src * n_tok * d_model, bytes_accessed=8 * n_src * n_tok * d_model, transcendentals=0),
        name="combine_rows",
    )(table, cols, y_rows)


def finish_kernel(*refs):
    h_ref, shared_ref, routed_ref, out_ref = refs[-4:]
    total = h_ref[...].astype(jnp.float32) + shared_ref[...].astype(jnp.float32) + routed_ref[...]
    out_ref[...] = total.astype(jnp.bfloat16)


def finish_rows(unit, held, h, shared, routed, shape):
    n_micro, n_seq, seq_len, d_model = shape
    block = seq_len // 2
    base = (unit.micro * n_seq + unit.first) * 2
    rows = pl.BlockSpec((block, d_model), lambda i: (i, 0))
    before = [] if held is None else [held]
    return pl.pallas_call(
        finish_kernel,
        out_shape=jax.ShapeDtypeStruct((n_micro * n_seq * seq_len, d_model), jnp.bfloat16),
        grid=(unit.count * 2,),
        in_specs=[pl.BlockSpec(memory_space=pl.ANY)] * len(before) + [rows, rows, rows],
        out_specs=pl.BlockSpec((block, d_model), lambda i: (base + i, 0)),
        input_output_aliases={0: 0} if before else {},
        compiler_params=pltpu.CompilerParams(dimension_semantics=("arbitrary",)),
        cost_estimate=pl.CostEstimate(flops=3 * unit.count * seq_len * d_model, bytes_accessed=10 * unit.count * seq_len * d_model, transcendentals=0),
        name="finish_rows",
    )(*before, h, shared, routed)


def solution(mesh):
    group_size = mesh.shape["ep"]
    n_src = group_size // 2
    ring_groups = [[2 * k + core for k in range(n_src)] for core in range(2)]
    pair_perm = [(k, k ^ 1) for k in range(group_size)]
    up_perm = [(k, (k + 2) % group_size) for k in range(group_size)]
    down_perm = [(k, (k - 2) % group_size) for k in range(group_size)]

    def device_step(tokens, expert_ids, route_weights, attn_norm, w_query, w_key, w_value, w_out, ffn_norm, w_gate, w_up, w_down, shared_gate, shared_up, shared_down):
        n_micro, n_seq, seq_len, d_model = tokens.shape
        n_tok = n_seq * seq_len
        top_count = expert_ids.shape[-1]
        half = w_gate.shape[0]
        n_local = 2 * half
        slot_cap = capacity_of(n_tok, top_count, half * group_size)
        max_rows = n_local * slot_cap
        me = lax.axis_index("ep")

        own = (w_gate, w_up, w_down)
        other = tuple(lax.ppermute(w, "ep", pair_perm) for w in own)

        meta = jnp.concatenate([expert_ids.astype(jnp.float32).transpose(0, 2, 1), route_weights.transpose(0, 2, 1), jnp.zeros((n_micro, 16 - 2 * top_count, n_tok), jnp.float32)], axis=1)
        meta = lax.all_gather(meta.reshape(n_micro * 16, n_tok), "ep", axis=0, tiled=True)
        slots, cols, table = route_rows(meta, me.reshape(1).astype(jnp.int32), half, top_count, n_src, n_micro, n_seq, seq_len)
        table = jnp.concatenate([table.reshape(-1), jnp.broadcast_to(me.astype(jnp.int32), (PIECE,))])

        gains = (attn_norm.reshape(1, d_model), ffn_norm.reshape(1, d_model))
        attn_weights = (w_query.transpose(1, 0, 2), w_key.transpose(1, 0, 2), w_value.transpose(1, 0, 2), w_out)
        units = [Unit(0, q, 1, n_src, n_seq) for q in range(n_seq)] + [Unit(m, 0, n_seq, n_src, n_seq) for m in range(1, n_micro)]
        hs, zs, gathered = [], [], []
        for unit in units:
            if zs:
                tokens, _ = lax.optimization_barrier((tokens, zs[-1]))
            h, z = attention_rows(tokens, unit.micro, unit.first, unit.count, gains, attn_weights)
            hs.append(h.reshape(-1, d_model))
            zs.append(z.reshape(-1, d_model))
            if unit.count == 1 or not BY_HOPS:
                gathered.append([lax.all_gather(zs[-1], "ep", axis=0, tiled=True, axis_index_groups=ring_groups)])
            else:
                left = [lax.ppermute(z[q], "ep", up_perm) for q in range(n_seq)]
                right = [lax.ppermute(z[q], "ep", down_perm) for q in range(n_seq)]
                far = [lax.ppermute(left[q], "ep", up_perm) if q % 2 == 0 else lax.ppermute(right[q], "ep", down_perm) for q in range(n_seq)]
                gathered.append([z, *left, *right, *far])
        out, partial = None, None
        routed, shared = [], []
        for k, unit in enumerate(units):
            if partial is not None:
                table, _ = lax.optimization_barrier((table, partial))
            x_rows = gather_rows(unit, table, slots, gathered[k], n_local, top_count, max_rows)
            seg_rows = (slot_cap + (SEG * unit.count if unit.count > 1 else 0)) * n_src
            y_rows = expert_rows(unit, table, x_rows, own, other, -(-seg_rows // ROWS) * ROWS)
            partial = combine_rows(unit, table, cols, y_rows, n_local, top_count)
            routed.append(lax.psum_scatter(partial, "ep", scatter_dimension=0, tiled=True, axis_index_groups=ring_groups))
        for k, unit in enumerate(units):
            shared.append(swiglu(zs[k], shared_gate, shared_up, shared_down))
        for k, unit in enumerate(units):
            out = finish_rows(unit, out, hs[k], shared[k], routed[k], tokens.shape)
        return out.reshape(tokens.shape)

    token_spec = P(None, ("dp", "ep"), None, None)
    route_spec = P(None, ("dp", "ep"), None)
    rep_spec = P()
    expert_spec = P("ep", None, None)
    in_specs = (token_spec, route_spec, route_spec, rep_spec, rep_spec, rep_spec, rep_spec, rep_spec, rep_spec, expert_spec, expert_spec, expert_spec, rep_spec, rep_spec, rep_spec)

    return jax.shard_map(device_step, mesh=mesh, in_specs=in_specs, out_specs=token_spec, check_vma=False)
```

```python
import functools

import jax
import jax.numpy as jnp
from jax import lax
from jax.experimental import pallas as pl
from jax.experimental.pallas import tpu as pltpu
from jax.sharding import PartitionSpec as P


NORM_EPS = 1e-6
CAP_FACTOR = 2
SLOT_ALIGN = 8
SEG = 16
ROWS = 256
Q_BLOCKS = 1
FIELD = 128
PIECE = 8 * FIELD
BY_HOPS = True
VMEM_LIMIT = 64_000_000


def capacity_of(n_tok, top_count, experts):
    return SLOT_ALIGN * ((CAP_FACTOR * n_tok * top_count + SLOT_ALIGN * experts - 1) // (SLOT_ALIGN * experts))


def rms_norm(in_vals, norm_gain):
    wide_vals = in_vals.astype(jnp.float32)
    inv_rms = lax.rsqrt(jnp.mean(wide_vals * wide_vals, axis=-1, keepdims=True) + NORM_EPS)
    return (wide_vals * inv_rms * norm_gain.astype(jnp.float32)).astype(jnp.bfloat16)


def attention_kernel(gains_ref, x_ref, wq_ref, wk_ref, wv_ref, wo_ref, h_ref, *refs):
    group, seq = pl.program_id(0), pl.program_id(1)
    *z_refs, normed, acc = refs
    seq_len, d_model = normed.shape[1:]
    per, _, head_dim = wq_ref.shape
    block = seq_len // Q_BLOCKS

    @pl.when(group == 0)
    def _():
        normed[seq] = rms_norm(x_ref[0, seq], gains_ref[0:1, :])

    rows = normed[seq]
    project = lambda w_ref: jnp.dot(rows, jnp.concatenate([w_ref[i] for i in range(per)], axis=1), preferred_element_type=jnp.float32).astype(jnp.bfloat16)
    queries, key_rows, value_rows = project(wq_ref), project(wk_ref), project(wv_ref)
    above = lax.broadcasted_iota(jnp.int32, (block, block), 0) < lax.broadcasted_iota(jnp.int32, (block, block), 1)
    heads = []
    for i in range(per):
        lanes = slice(i * head_dim, (i + 1) * head_dim)
        k, v = key_rows[:, lanes], value_rows[:, lanes]
        outs = []
        for part in range(Q_BLOCKS):
            q = queries[part * block : (part + 1) * block, lanes]
            scores = lax.dot_general(q, k[: (part + 1) * block], (((1,), (1,)), ((), ())), preferred_element_type=jnp.float32) * (head_dim**-0.5)
            diag = jnp.where(above, -jnp.inf, scores[:, part * block :])
            scores = diag if part == 0 else jnp.concatenate([scores[:, : part * block], diag], axis=1)
            shifted = jnp.exp(scores - jnp.max(scores, axis=1, keepdims=True))
            probs = (shifted * (1.0 / jnp.sum(shifted, axis=1, keepdims=True))).astype(jnp.bfloat16)
            outs.append(jnp.dot(probs, v[: (part + 1) * block], preferred_element_type=jnp.float32).astype(jnp.bfloat16))
        heads.append(jnp.concatenate(outs, axis=0))
    mix = jnp.concatenate(heads, axis=1)
    added = jnp.dot(mix, wo_ref[...].reshape(per * head_dim, d_model), preferred_element_type=jnp.float32)

    @pl.when(group == 0)
    def _():
        acc[seq] = added

    @pl.when(group > 0)
    def _():
        acc[seq] += added

    @pl.when(group == pl.num_programs(0) - 1)
    def _():
        residual = (x_ref[0, seq].astype(jnp.float32) + acc[seq]).astype(jnp.bfloat16)
        h_ref[seq] = residual
        z = rms_norm(residual, gains_ref[1:2, :])
        for i, z_ref in enumerate(z_refs):

            @pl.when(seq == i)
            def _():
                z_ref[...] = z


def attention_rows(tokens, micro, first, n_seq, gains, weights):
    _, _, seq_len, d_model = tokens.shape
    n_heads, _, head_dim = weights[0].shape
    per = 4 if n_heads % 4 == 0 else 1
    out = jax.ShapeDtypeStruct((n_seq, seq_len, d_model), jnp.bfloat16)
    whole = pl.BlockSpec((n_seq, seq_len, d_model), lambda g, s: (0, 0, 0))
    gain = pl.BlockSpec((2, d_model), lambda g, s: (0, 0))
    z_out = pl.BlockSpec((seq_len, d_model), lambda g, s: (0, 0))
    in_w = pl.BlockSpec((per, d_model, head_dim), lambda g, s: (g, 0, 0))
    rows = n_seq * seq_len
    return pl.pallas_call(
        attention_kernel,
        out_shape=(out, *[jax.ShapeDtypeStruct((seq_len, d_model), jnp.bfloat16)] * n_seq),
        grid=(n_heads // per, n_seq),
        in_specs=[gain, pl.BlockSpec((1, n_seq, seq_len, d_model), lambda g, s: (micro, first // n_seq, 0, 0)), in_w, in_w, in_w, pl.BlockSpec((per, head_dim, d_model), lambda g, s: (g, 0, 0))],
        out_specs=(whole, *[z_out] * n_seq),
        scratch_shapes=[pltpu.VMEM((n_seq, seq_len, d_model), jnp.bfloat16), pltpu.VMEM((n_seq, seq_len, d_model), jnp.float32)],
        compiler_params=pltpu.CompilerParams(dimension_semantics=("arbitrary", "arbitrary"), vmem_limit_bytes=VMEM_LIMIT),
        cost_estimate=pl.CostEstimate(flops=8 * rows * d_model * d_model, bytes_accessed=30_000_000, transcendentals=0),
        name="attention_rows",
    )(gains, tokens, *weights)


def swiglu(in_rows, gate_w, up_w, down_w):
    gate_act = jnp.dot(in_rows, gate_w, preferred_element_type=jnp.float32)
    up_act = jnp.dot(in_rows, up_w, preferred_element_type=jnp.float32)
    hidden = (jax.nn.silu(gate_act) * up_act).astype(jnp.bfloat16)
    return jnp.dot(hidden, down_w, preferred_element_type=jnp.float32).astype(jnp.bfloat16)


def route_kernel(half, top_count, me_ref, meta_ref, slots_ref, cols_ref, table_ref, upper, placed):
    micro, src, seq = (pl.program_id(i) for i in range(3))
    me = me_ref[0]
    n_local, n_tok = 2 * half, upper.shape[0]
    acc = jnp.where(micro == 0, seq, 0)

    @pl.when((micro == 0) & (src == 0) & (seq == 0))
    def _():
        below = lax.broadcasted_iota(jnp.int32, upper.shape, 0) <= lax.broadcasted_iota(jnp.int32, upper.shape, 1)
        upper[...] = jnp.where(below, 1.0, 0.0).astype(jnp.bfloat16)

    @pl.when((src == 0) & ((micro == 0) | (seq == 0)))
    def _():
        placed[acc] = jnp.zeros(placed.shape[1:], jnp.float32)

    ids = meta_ref[0:top_count, :].astype(jnp.int32)
    from_own, from_other = ids - half * me, ids - half * (me ^ 1)
    local = jnp.where((from_own >= 0) & (from_own < half), from_own, jnp.where((from_other >= 0) & (from_other < half), from_other + half, -1))
    expert_at = lax.broadcasted_iota(jnp.int32, (n_local, n_tok), 0)
    hits = [local[j : j + 1, :] == expert_at for j in range(top_count)]
    mask = jnp.where(functools.reduce(jnp.logical_or, hits), 1.0, 0.0)
    bits = mask.astype(jnp.bfloat16)
    running = jnp.dot(bits, upper[...], preferred_element_type=jnp.float32)
    pad = lambda counts: jnp.floor((counts + (SEG - 1)) * (1.0 / SEG))
    units = jnp.broadcast_to(pad(running[:, n_tok - 1 : n_tok]), (n_local, FIELD)).astype(jnp.bfloat16)
    before = lax.broadcasted_iota(jnp.int32, (n_local, n_local), 1) < lax.broadcasted_iota(jnp.int32, (n_local, n_local), 0)
    offs = jnp.dot(jnp.where(before, 1.0, 0.0).astype(jnp.bfloat16), units, preferred_element_type=jnp.float32) * SEG
    row_of = offs[:, 0:1] + running
    slots = [jnp.sum(jnp.where(hit, row_of, 0.0), axis=0, keepdims=True) - 1.0 for hit in hits]
    none = jnp.full((1, n_tok), -1.0, jnp.float32)
    slots_ref[...] = jnp.concatenate(slots + [none] * (8 - top_count), axis=0).astype(jnp.int32)
    cols_ref[...] = jnp.concatenate(slots + [meta_ref[top_count : 2 * top_count, :]] + [none] * (16 - 2 * top_count), axis=0)
    wide = jnp.concatenate([bits, jnp.zeros((FIELD - n_local, n_tok), jnp.bfloat16)], axis=0)
    counts = lax.dot_general(jnp.ones((8, n_tok), jnp.bfloat16), wide, (((1,), (1,)), ((), ())), preferred_element_type=jnp.float32)
    units_row = pad(counts)
    before_row = lax.broadcasted_iota(jnp.int32, (FIELD, FIELD), 0) < lax.broadcasted_iota(jnp.int32, (FIELD, FIELD), 1)
    offs_row = jnp.dot(units_row.astype(jnp.bfloat16), jnp.where(before_row, 1.0, 0.0).astype(jnp.bfloat16), preferred_element_type=jnp.float32) * SEG
    sizes_row = units_row * SEG
    at = lax.broadcasted_iota(jnp.int32, (8, FIELD), 0)
    fields = jnp.where(at == 0, offs_row, jnp.where(at == 1, sizes_row, placed[acc]))
    table_ref[...] = fields.astype(jnp.int32)
    placed[acc] = placed[acc] + sizes_row


def route_rows(meta, me, half, top_count, n_src, n_micro, n_seq, seq_len):
    spot = lambda m, s, q, t: (m, s, q, 0, 0)
    piece = lambda rows, lanes, dtype: (jax.ShapeDtypeStruct((n_micro, n_src, n_seq, rows, lanes), dtype), pl.BlockSpec((None, None, None, rows, lanes), spot))
    outs = [piece(8, seq_len, jnp.int32), piece(16, seq_len, jnp.float32), piece(8, FIELD, jnp.int32)]
    return pl.pallas_call(
        functools.partial(route_kernel, half, top_count),
        out_shape=tuple(o[0] for o in outs),
        grid_spec=pltpu.PrefetchScalarGridSpec(
            num_scalar_prefetch=1,
            grid=(n_micro, n_src, n_seq),
            in_specs=[pl.BlockSpec((16, seq_len), lambda m, s, q, t: ((2 * s + lax.rem(t[0], 2)) * n_micro + m, q))],
            out_specs=tuple(o[1] for o in outs),
            scratch_shapes=[pltpu.VMEM((seq_len, seq_len), jnp.bfloat16), pltpu.VMEM((n_seq, 8, FIELD), jnp.float32)],
        ),
        compiler_params=pltpu.CompilerParams(dimension_semantics=("arbitrary",) * 3),
        cost_estimate=pl.CostEstimate(flops=500_000_000, bytes_accessed=2_000_000, transcendentals=0),
        name="route_rows",
    )(me, meta)


class Unit:
    def __init__(self, micro, first, count, n_src, n_seq):
        self.micro, self.first, self.count, self.n_src, self.n_seq = micro, first, count, n_src, n_seq
        self.pieces = n_src * count

    def spot(self, i):
        return self.micro, i // self.count, self.first + i % self.count

    def field(self, table_ref, i, which, expert):
        micro, src, seq = self.spot(i)
        return table_ref[((micro * self.n_src + src) * self.n_seq + seq) * PIECE + which * FIELD + expert]

    def rows_of(self, table_ref, i, n_local):
        return self.field(table_ref, i, 0, n_local - 1) + self.field(table_ref, i, 1, n_local - 1)

    def spec(self, rows, lanes):
        return pl.BlockSpec((None, None, None, rows, lanes), lambda i, *_: (*self.spot(i), 0, 0))


def gather_kernel(unit, n_local, top_count, table_ref, slots_ref, *refs):
    z_refs, (x_hbm, buf, sems, sent) = refs[: -4 if len(refs) == 5 else -6], (refs[-4:] if len(refs) == 5 else refs[-6:-2])
    src = pl.program_id(0)
    total = unit.rows_of(table_ref, src, n_local)
    block = buf.shape[1]
    n_tok = slots_ref.shape[1]
    if len(refs) == 5:
        z = z_refs[0]
    else:
        z_buf, z_sems = refs[-2:]
        x_at = table_ref[table_ref.shape[0] - 1] // 2

        def fetch(i):
            _, s, q = unit.spot(i)
            away = lax.rem(s - x_at + unit.n_src, unit.n_src)
            own, left, right, far = (z_refs[g * unit.count : (g + 1) * unit.count] for g in range(4))
            for seq in range(unit.count):
                for hop, ref in enumerate((own[seq], right[seq], far[seq], left[seq])):

                    @pl.when((q == seq) & (away == hop))
                    def _():
                        pltpu.make_async_copy(ref, z_buf.at[i & 1], z_sems.at[i & 1]).start()

        @pl.when(src == 0)
        def _():
            fetch(src)

        @pl.when(src + 1 < unit.pieces)
        def _():
            fetch(src + 1)

        pltpu.make_async_copy(z_refs[1], z_buf.at[src & 1], z_sems.at[src & 1]).wait()
        z = z_buf.at[src & 1]

    @pl.when(src == 0)
    def _():
        sent[0] = 0

    def copy(slot, row):
        return pltpu.make_async_copy(buf.at[slot], x_hbm.at[src, pl.ds(row, block)], sems.at[slot])

    def chunk(c, carry):
        base = pl.multiple_of(c * block, block)
        slot = sent[0] & 1

        @pl.when(sent[0] >= 2)
        def _():
            copy(slot, 0).wait()

        for part in range(block // ROWS):
            rows = lax.broadcasted_iota(jnp.int32, (ROWS, n_tok), 0) + (base + part * ROWS)
            hit = rows == slots_ref[0:1, :]
            for j in range(1, top_count):
                hit = hit | (rows == slots_ref[j : j + 1, :])
            pick = jnp.where(hit, 1.0, 0.0).astype(jnp.bfloat16)
            got = jnp.dot(pick, z[...], preferred_element_type=jnp.float32)
            buf[slot, part * ROWS : (part + 1) * ROWS, :] = got.astype(jnp.bfloat16)
        copy(slot, base).start()
        sent[0] = sent[0] + 1
        return carry

    lax.fori_loop(0, (total + block - 1) // block, chunk, 0)

    @pl.when(src == unit.pieces - 1)
    def _():
        for back in (1, 2):

            @pl.when(sent[0] >= back)
            def _():
                copy((sent[0] - back) & 1, 0).wait()


def gather_rows(unit, table, slots, zs, n_local, top_count, max_rows):
    n_tok = slots.shape[-1]
    d_model = zs[0].shape[-1]
    block = 2 * ROWS
    held = len(zs) > 1
    z_specs = [pl.BlockSpec(memory_space=pl.ANY)] * len(zs) if held else [pl.BlockSpec((n_tok, d_model), lambda i, t: (i, 0))]
    scratch = [pltpu.VMEM((2, block, d_model), jnp.bfloat16), pltpu.SemaphoreType.DMA((2,)), pltpu.SMEM((1,), jnp.int32)]
    if held:
        scratch += [pltpu.VMEM((2, n_tok, d_model), jnp.bfloat16), pltpu.SemaphoreType.DMA((2,))]
    return pl.pallas_call(
        functools.partial(gather_kernel, unit, n_local, top_count),
        out_shape=jax.ShapeDtypeStruct((unit.pieces, -(-max_rows // block) * block, d_model), jnp.bfloat16),
        grid_spec=pltpu.PrefetchScalarGridSpec(
            num_scalar_prefetch=1,
            grid=(unit.pieces,),
            in_specs=[unit.spec(8, n_tok), *z_specs],
            out_specs=pl.BlockSpec(memory_space=pl.ANY),
            scratch_shapes=scratch,
        ),
        compiler_params=pltpu.CompilerParams(dimension_semantics=("arbitrary",), vmem_limit_bytes=VMEM_LIMIT),
        cost_estimate=pl.CostEstimate(flops=2 * 1024 * unit.pieces * n_tok * d_model, bytes_accessed=6 * unit.pieces * n_tok * d_model, transcendentals=0),
        name="gather_rows",
    )(table, slots, *zs)


def expert_kernel(unit, n_local, table_ref, x_hbm, ga, ua, da, gb, ub, db, y_hbm, x_buf, y_buf, in_sems, out_sems):
    step = pl.program_id(0)

    def pieces(which, act):
        slot = lax.rem(which, 2)
        for s in range(unit.pieces):
            off, size, place = (pl.multiple_of(unit.field(table_ref, s, f, which), SEG) for f in range(3))
            act(slot, s, off, place, size)

    def in_copy(slot, s, off, place, size):
        return pltpu.make_async_copy(x_hbm.at[s, pl.ds(off, size)], x_buf.at[slot, pl.ds(place, size)], in_sems.at[slot, s])

    def out_copy(slot, s, off, place, size):
        return pltpu.make_async_copy(y_buf.at[slot, pl.ds(place, size)], y_hbm.at[s, pl.ds(off, size)], out_sems.at[slot, s])

    @pl.when(step == 0)
    def _():
        pieces(step, lambda *a: in_copy(*a).start())

    @pl.when(step + 1 < n_local)
    def _():
        pieces(step + 1, lambda *a: in_copy(*a).start())

    pieces(step, lambda *a: in_copy(*a).wait())

    @pl.when(step >= 2)
    def _():
        pieces(step - 2, lambda *a: out_copy(*a).wait())

    slot = lax.rem(step, 2)
    total = unit.field(table_ref, unit.pieces - 1, 1, step) + unit.field(table_ref, unit.pieces - 1, 2, step)
    n_blocks = (total + ROWS // 2 - 1) // ROWS

    def run(gate, up, down):
        def feed(start, size):
            rows = pl.ds(pl.multiple_of(start, ROWS), size)
            x = x_buf[slot, rows, :]
            g = jnp.dot(x, gate[0], preferred_element_type=jnp.float32)
            u = jnp.dot(x, up[0], preferred_element_type=jnp.float32)
            h = (g * jax.nn.sigmoid(g) * u).astype(jnp.bfloat16)
            y_buf[slot, rows, :] = jnp.dot(h, down[0], preferred_element_type=jnp.float32).astype(jnp.bfloat16)

        def block(c, carry):
            feed(c * ROWS, ROWS)
            return carry

        lax.fori_loop(0, n_blocks, block, 0)

        @pl.when(total > n_blocks * ROWS)
        def _():
            feed(n_blocks * ROWS, ROWS // 2)

    @pl.when(step < n_local // 2)
    def _():
        run(ga, ua, da)

    @pl.when(step >= n_local // 2)
    def _():
        run(gb, ub, db)

    pieces(step, lambda *a: out_copy(*a).start())

    @pl.when(step == n_local - 1)
    def _():
        pieces(step - 1, lambda *a: out_copy(*a).wait())
        pieces(step, lambda *a: out_copy(*a).wait())


def expert_rows(unit, table, x_rows, own, other, buf_rows):
    n_src, _, d_model = x_rows.shape
    half, _, width = own[0].shape
    n_local = 2 * half
    own_at = lambda l, t: (jnp.minimum(l, half - 1), 0, 0)
    other_at = lambda l, t: (jnp.maximum(l - half, 0), 0, 0)
    return pl.pallas_call(
        functools.partial(expert_kernel, unit, n_local),
        out_shape=jax.ShapeDtypeStruct(x_rows.shape, jnp.bfloat16),
        grid_spec=pltpu.PrefetchScalarGridSpec(
            num_scalar_prefetch=1,
            grid=(n_local,),
            in_specs=[
                pl.BlockSpec(memory_space=pl.ANY),
                pl.BlockSpec((1, d_model, width), own_at),
                pl.BlockSpec((1, d_model, width), own_at),
                pl.BlockSpec((1, width, d_model), own_at),
                pl.BlockSpec((1, d_model, width), other_at),
                pl.BlockSpec((1, d_model, width), other_at),
                pl.BlockSpec((1, width, d_model), other_at),
            ],
            out_specs=pl.BlockSpec(memory_space=pl.ANY),
            scratch_shapes=[
                pltpu.VMEM((2, buf_rows, d_model), jnp.bfloat16),
                pltpu.VMEM((2, buf_rows, d_model), jnp.bfloat16),
                pltpu.SemaphoreType.DMA((2, n_src)),
                pltpu.SemaphoreType.DMA((2, n_src)),
            ],
        ),
        compiler_params=pltpu.CompilerParams(dimension_semantics=("arbitrary",), vmem_limit_bytes=VMEM_LIMIT),
        cost_estimate=pl.CostEstimate(flops=2 * 8192 * d_model * width * 3, bytes_accessed=115_000_000, transcendentals=0),
        name="expert_rows",
    )(table, x_rows, *own, *other)


def combine_kernel(unit, n_local, top_count, table_ref, cols_ref, y_hbm, out_ref, slot_bc, weight_bc, buf, sems):
    src = pl.program_id(0)
    n_tok = out_ref.shape[0]
    n_src = unit.pieces
    total = unit.rows_of(table_ref, src, n_local)
    n_chunks = (total + ROWS - 1) // ROWS
    lanes = 128
    ahead = 2 + (src & 1)

    def copy(which, c, slot):
        return pltpu.make_async_copy(y_hbm.at[which, pl.ds(pl.multiple_of(c * ROWS, ROWS), ROWS)], buf.at[slot], sems.at[slot])

    @pl.when(src == 0)
    def _():
        copy(src, 0, ahead).start()

    @pl.when(src + 1 < n_src)
    def _():
        copy(src + 1, 0, 5 - ahead).start()

    @pl.when(n_chunks > 1)
    def _():
        copy(src, 1, 1).start()

    cols = cols_ref[...].T
    for j in range(top_count):
        slot_bc[j] = jnp.broadcast_to(cols[:, j : j + 1], (n_tok, lanes))
        weight_bc[j] = jnp.broadcast_to(cols[:, top_count + j : top_count + j + 1], (n_tok, lanes))
    out_ref[...] = jnp.zeros_like(out_ref)
    copy(src, 0, ahead).wait()

    def chunk(c, carry):
        base = c * ROWS
        slot = jnp.where(c == 0, ahead, c & 1)

        @pl.when(c > 0)
        def _():
            copy(src, c, slot).wait()

        @pl.when((c > 0) & (c + 1 < n_chunks))
        def _():
            copy(src, c + 1, (c + 1) & 1).start()

        y = buf[slot]
        y_at = lax.broadcasted_iota(jnp.int32, y.shape, 0) + base
        y = jnp.where(y_at < total, y, jnp.zeros_like(y))
        for i in range(n_tok // ROWS):
            tok = slice(i * ROWS, (i + 1) * ROWS)
            parts = [[], [], []]
            for half in range(ROWS // lanes):
                lane_at = (lax.broadcasted_iota(jnp.int32, (ROWS, lanes), 1) + (base + half * lanes)).astype(jnp.float32)
                coef = jnp.zeros((ROWS, lanes), jnp.float32)
                for j in range(top_count):
                    coef = jnp.where(slot_bc[j, tok, :] == lane_at, weight_bc[j, tok, :], coef)
                high = coef.astype(jnp.bfloat16)
                rest = coef - high.astype(jnp.float32)
                mid = rest.astype(jnp.bfloat16)
                low = (rest - mid.astype(jnp.float32)).astype(jnp.bfloat16)
                for part, val in zip(parts, (high, mid, low)):
                    part.append(val)
            high, mid, low = (jnp.concatenate(part, axis=1) for part in parts)
            acc = jnp.dot(low, y, preferred_element_type=jnp.float32)
            acc = acc + jnp.dot(mid, y, preferred_element_type=jnp.float32)
            acc = acc + jnp.dot(high, y, preferred_element_type=jnp.float32)
            out_ref[tok, :] += acc
        return carry

    lax.fori_loop(0, n_chunks, chunk, 0)


def combine_rows(unit, table, cols, y_rows, n_local, top_count):
    n_src, _, d_model = y_rows.shape
    n_tok = cols.shape[-1]
    return pl.pallas_call(
        functools.partial(combine_kernel, unit, n_local, top_count),
        out_shape=jax.ShapeDtypeStruct((n_src * n_tok, d_model), jnp.float32),
        grid_spec=pltpu.PrefetchScalarGridSpec(
            num_scalar_prefetch=1,
            grid=(n_src,),
            in_specs=[
                unit.spec(16, n_tok),
                pl.BlockSpec(memory_space=pl.ANY),
            ],
            out_specs=pl.BlockSpec((n_tok, d_model), lambda s, t: (s, 0)),
            scratch_shapes=[
                pltpu.VMEM((top_count, n_tok, 128), jnp.float32),
                pltpu.VMEM((top_count, n_tok, 128), jnp.float32),
                pltpu.VMEM((4, ROWS, d_model), jnp.bfloat16),
                pltpu.SemaphoreType.DMA((4,)),
            ],
        ),
        compiler_params=pltpu.CompilerParams(dimension_semantics=("arbitrary",), vmem_limit_bytes=VMEM_LIMIT),
        cost_estimate=pl.CostEstimate(flops=6 * 1024 * n_src * n_tok * d_model, bytes_accessed=8 * n_src * n_tok * d_model, transcendentals=0),
        name="combine_rows",
    )(table, cols, y_rows)


def finish_kernel(*refs):
    h_ref, shared_ref, routed_ref, out_ref = refs[-4:]
    total = h_ref[...].astype(jnp.float32) + shared_ref[...].astype(jnp.float32) + routed_ref[...]
    out_ref[...] = total.astype(jnp.bfloat16)


def finish_rows(unit, held, h, shared, routed, shape):
    n_micro, n_seq, seq_len, d_model = shape
    block = seq_len // 2
    base = (unit.micro * n_seq + unit.first) * 2
    rows = pl.BlockSpec((block, d_model), lambda i: (i, 0))
    before = [] if held is None else [held]
    return pl.pallas_call(
        finish_kernel,
        out_shape=jax.ShapeDtypeStruct((n_micro * n_seq * seq_len, d_model), jnp.bfloat16),
        grid=(unit.count * 2,),
        in_specs=[pl.BlockSpec(memory_space=pl.ANY)] * len(before) + [rows, rows, rows],
        out_specs=pl.BlockSpec((block, d_model), lambda i: (base + i, 0)),
        input_output_aliases={0: 0} if before else {},
        compiler_params=pltpu.CompilerParams(dimension_semantics=("arbitrary",)),
        cost_estimate=pl.CostEstimate(flops=3 * unit.count * seq_len * d_model, bytes_accessed=10 * unit.count * seq_len * d_model, transcendentals=0),
        name="finish_rows",
    )(*before, h, shared, routed)


def solution(mesh):
    group_size = mesh.shape["ep"]
    n_src = group_size // 2
    ring_groups = [[2 * k + core for k in range(n_src)] for core in range(2)]
    pair_perm = [(k, k ^ 1) for k in range(group_size)]
    up_perm = [(k, (k + 2) % group_size) for k in range(group_size)]
    down_perm = [(k, (k - 2) % group_size) for k in range(group_size)]

    def device_step(tokens, expert_ids, route_weights, attn_norm, w_query, w_key, w_value, w_out, ffn_norm, w_gate, w_up, w_down, shared_gate, shared_up, shared_down):
        n_micro, n_seq, seq_len, d_model = tokens.shape
        n_tok = n_seq * seq_len
        top_count = expert_ids.shape[-1]
        half = w_gate.shape[0]
        n_local = 2 * half
        slot_cap = capacity_of(n_tok, top_count, half * group_size)
        max_rows = n_local * slot_cap
        me = lax.axis_index("ep")

        own = (w_gate, w_up, w_down)
        other = tuple(lax.ppermute(w, "ep", pair_perm) for w in own)

        meta = jnp.concatenate([expert_ids.astype(jnp.float32).transpose(0, 2, 1), route_weights.transpose(0, 2, 1), jnp.zeros((n_micro, 16 - 2 * top_count, n_tok), jnp.float32)], axis=1)
        meta = lax.all_gather(meta.reshape(n_micro * 16, n_tok), "ep", axis=0, tiled=True)
        slots, cols, table = route_rows(meta, me.reshape(1).astype(jnp.int32), half, top_count, n_src, n_micro, n_seq, seq_len)
        table = jnp.concatenate([table.reshape(-1), jnp.broadcast_to(me.astype(jnp.int32), (PIECE,))])

        gains = jnp.stack([attn_norm, ffn_norm]).astype(jnp.float32)
        attn_weights = (w_query.transpose(1, 0, 2), w_key.transpose(1, 0, 2), w_value.transpose(1, 0, 2), w_out)
        units = [Unit(0, q, 1, n_src, n_seq) for q in range(n_seq)] + [Unit(m, 0, n_seq, n_src, n_seq) for m in range(1, n_micro)]
        hs, zs, gathered = [], [], []
        for unit in units:
            if zs:
                tokens, _ = lax.optimization_barrier((tokens, zs[-1][0]))
            h, *z = attention_rows(tokens, unit.micro, unit.first, unit.count, gains, attn_weights)
            hs.append(h.reshape(-1, d_model))
            zs.append(z)
            if unit.count == 1 or not BY_HOPS:
                gathered.append([lax.all_gather(jnp.concatenate(z) if unit.count > 1 else z[0], "ep", axis=0, tiled=True, axis_index_groups=ring_groups)])
            else:
                left = [lax.ppermute(z[q], "ep", up_perm) for q in range(n_seq)]
                right = [lax.ppermute(z[q], "ep", down_perm) for q in range(n_seq)]
                far = [lax.ppermute(left[q], "ep", up_perm) if q % 2 == 0 else lax.ppermute(right[q], "ep", down_perm) for q in range(n_seq)]
                gathered.append([*z, *left, *right, *far])
        out, partial = None, None
        routed, shared = [], []
        for k, unit in enumerate(units):
            if partial is not None:
                table, _ = lax.optimization_barrier((table, partial))
            x_rows = gather_rows(unit, table, slots, gathered[k], n_local, top_count, max_rows)
            seg_rows = (slot_cap + (SEG * unit.count if unit.count > 1 else 0)) * n_src
            y_rows = expert_rows(unit, table, x_rows, own, other, -(-seg_rows // ROWS) * ROWS)
            partial = combine_rows(unit, table, cols, y_rows, n_local, top_count)
            routed.append(lax.psum_scatter(partial, "ep", scatter_dimension=0, tiled=True, axis_index_groups=ring_groups))
        for k, unit in enumerate(units):
            shared.append(swiglu(jnp.concatenate(zs[k]) if unit.count > 1 else zs[k][0], shared_gate, shared_up, shared_down))
        for k, unit in enumerate(units):
            out = finish_rows(unit, out, hs[k], shared[k], routed[k], tokens.shape)
        return out.reshape(tokens.shape)

    token_spec = P(None, ("dp", "ep"), None, None)
    route_spec = P(None, ("dp", "ep"), None)
    rep_spec = P()
    expert_spec = P("ep", None, None)
    in_specs = (token_spec, route_spec, route_spec, rep_spec, rep_spec, rep_spec, rep_spec, rep_spec, rep_spec, expert_spec, expert_spec, expert_spec, rep_spec, rep_spec, rep_spec)

    return jax.shard_map(device_step, mesh=mesh, in_specs=in_specs, out_specs=token_spec, check_vma=False)
```
